256 devices in a mesh: section: 32 (over z, y), dp: 4 (over x), mp: 2 (over core).
Axes of the slice: x: 4, y: 4, z: 8, core: 2. Of those that a mesh axis runs over, the one named last changes fastest.
Arguments:
- inputs: bfloat16 [4, 128, 8192], P(None, 'dp'), may hold values from -12.7 to 12.7
- value_weight: bfloat16 [32, 8192, 1024], P('section', None, 'mp'), may hold values from -0.13975425 to 0.13975425
- carry_gain: float32 [32, 8192], P('section'), may hold values from 0.6 to 1.4
- channel_bins: int32 [32, 8192], P('section'), may hold values from 0 to 15
- grid_picks: int32 [32, 20], P('section'), may hold values from 0 to 19, each once within a row
Outputs:
- quant_out: bfloat16 [32, 4, 128, 1024], P('section', None, 'dp', 'mp')
- grid_loss: float32 [32, 4], P('section')
The draws below stay inside these ranges and needn't reach their ends.
Inputs may be any that keep to these rules, and one draw needn't show every extreme that they name: `grid_picks`: each row lists every grid point once.
All inputs are finite; a program needn't handle non-finite values.
Results may differ from the reference program's by a relative error of at most 0.029.
Values may be sent and summed in bfloat16 or wider, within the bound.
A program may use at most 192 MiB of HBM per device.

```python
import math
import jax
import jax.numpy as jnp
from jax import lax

D = 8192
KV = 1024
HEAD = 128
GROUP = 128
GRID = 20
PICKS = 4
MICRO = 4
TOKENS = 128
LAYERS = 32


def draw_inputs(key, part):
    first_key = jax.random.fold_in(key, 11)
    position = jnp.arange(TOKENS, dtype=jnp.float32)
    row_scale = 10.0 ** (position / (TOKENS - 1) - 0.5)
    base = jnp.clip(jax.random.normal(first_key, (MICRO, TOKENS, D), dtype=jnp.float32), -4.0, 4.0)
    return (base * row_scale[None, :, None]).astype(jnp.bfloat16)


def draw_value_weight(key, part):
    first_key = jax.random.fold_in(key, 21)
    column = jnp.arange(KV, dtype=jnp.float32)
    column_scale = 10.0 ** (column / (KV - 1) - 0.5)
    base = jnp.clip(jax.random.normal(first_key, (LAYERS, D, KV), dtype=jnp.float32), -4.0, 4.0)
    return (base * column_scale[None, None, :] * D ** (-0.5)).astype(jnp.bfloat16)


def plant(result, rng, least, largest):
    extent = result.shape
    index_at = [jax.random.randint(jax.random.fold_in(rng, axis), (), 0, extent[axis]) for axis in range(len(extent))]
    result = result.at[tuple(index_at)].set(least)
    longest = extent.index(max(extent))
    index_at[longest] = (index_at[longest] + 1) % extent[longest]
    return result.at[tuple(index_at)].set(largest)


def setup_inputs(seed: int = 0) -> dict:
    streams_of = jax.random.split(jax.random.key(seed), 6)
    inputs = draw_inputs(jax.random.fold_in(streams_of[5], 71), 0)
    value_weight = draw_value_weight(jax.random.fold_in(streams_of[5], 71), 0)
    carry_gain = jnp.clip(1.0 + 0.08 * jax.random.normal(streams_of[2], (LAYERS, D), jnp.float32), 0.6, 1.4)
    channel_bins = plant(jax.random.randint(streams_of[3], (LAYERS, D), 0, 16), jax.random.fold_in(streams_of[3], 1), 0, 15).astype(jnp.int32)
    grid_picks = jax.vmap(lambda own: jax.random.permutation(own, GRID))(jax.random.split(streams_of[4], LAYERS)).reshape((LAYERS, GRID)).astype(jnp.int32)
    return dict(inputs=inputs, value_weight=value_weight, carry_gain=carry_gain, channel_bins=channel_bins, grid_picks=grid_picks)


EPS = 1e-06
LOSS_UNIT = 1000.0
TWO_PI = 2.0 * math.pi

def quantize(weight, channel_bin, grid_pick):
    exponent = grid_pick.astype(jnp.float32) / GRID
    scaling = jnp.exp2(exponent * channel_bin.astype(jnp.float32) / 4.0)
    scaled = weight.astype(jnp.float32) * scaling[:, None]
    blocks = scaled.reshape(scaled.shape[0] // GROUP, GROUP, scaled.shape[1])
    spacing = (lax.optimization_barrier(jnp.max(jnp.abs(blocks), axis=1, keepdims=True)) + EPS) / 7.0
    levels = blocks / spacing
    snapped = (levels - jnp.sin(TWO_PI * levels) / TWO_PI) * spacing
    return (snapped.reshape(scaled.shape) / scaling[:, None]).astype(jnp.bfloat16)

def repeat_heads(values):
    row_count, columns = values.shape
    head_view = values.reshape(row_count, columns // HEAD, 1, HEAD)
    spread = jnp.broadcast_to(head_view, (row_count, columns // HEAD, D // KV, HEAD))
    return spread.reshape(row_count, columns * (D // KV))

def reference(inputs, value_weight, carry_gain, channel_bins, grid_picks):
    residual_gain = 1.0 / math.sqrt(LAYERS)
    flat_rows = MICRO * TOKENS

    def layer_step(stream, layer_args):
        weight, gain_row, channel_bin, grid_row = layer_args
        exact = jnp.dot(stream, weight, preferred_element_type=jnp.float32)
        errors = []
        chosen = None
        for pick_index in range(PICKS):
            approx = jnp.dot(stream, quantize(weight, channel_bin, grid_row[pick_index]), preferred_element_type=jnp.float32)
            errors.append(jnp.sum(jnp.square(approx - exact)))
            if pick_index == 0:
                chosen = approx.astype(jnp.bfloat16)
        widened = repeat_heads(chosen)
        next_stream = (stream.astype(jnp.float32) * gain_row[None, :] + residual_gain * widened.astype(jnp.float32)).astype(jnp.bfloat16)
        losses = jnp.stack(errors) * LOSS_UNIT / (flat_rows * KV)
        return (next_stream, (chosen.reshape(MICRO, TOKENS, KV), losses))
    final_stream, outputs = lax.scan(layer_step, inputs.reshape(flat_rows, D), (value_weight, carry_gain, channel_bins, grid_picks))
    quant_out, grid_loss = outputs
    return (quant_out, grid_loss)
```

```python
import math

import jax
import jax.numpy as jnp
from jax import lax
from jax.experimental import pallas as pl
from jax.experimental.pallas import tpu as pltpu
from jax.sharding import PartitionSpec as P

D = 8192
KV = 1024
HALF = 512
HEAD = 128
GROUP = 128
GRID = 20
PICKS = 4
MICRO = 4
ROWS = 16
LATE = 16

EPS = 1e-06
LOSS_UNIT = 1000.0
MESH = pl.DeviceIdType.MESH
SINE = (
    0.9999996039221354,
    -6.579691570017649,
    12.98643600013728,
    -12.188101534445755,
    6.558042246424786,
    -1.953032018015784,
)
F32 = jnp.float32
BF16 = jnp.bfloat16


def sine_part(levels):
    r = levels - jnp.round(levels)
    z = r * r
    acc = jnp.full_like(z, SINE[-1])
    for c in SINE[-2::-1]:
        acc = acc * z + c
    return acc * r


def spread_rows(row_block, count, out):
    columns = row_block.T
    for k in range(count):
        out[k] = jnp.broadcast_to(columns[:, k : k + 1], (GROUP, 128))


def spacing_of(w_ref, scale, start, cs):
    high = None
    for q in range(4):
        part = w_ref[pl.ds(pl.multiple_of(start + 32 * q, 32), 32), cs].astype(F32) * scale(q)
        part = jnp.max(jnp.abs(part), axis=0, keepdims=True)
        high = part if high is None else jnp.maximum(high, part)
    return high + EPS


def first_body(w_ref, v_ref, q_ref, m_ref, acc, wide):
    acc[...] = jnp.zeros_like(acc)

    def block(r, carry):
        spread_rows(v_ref[r], 5, wide)
        start = r * GROUP
        for c in range(4):
            cs = pl.ds(c * 128, 128)
            high = spacing_of(w_ref, lambda q: wide[0, pl.ds(32 * q, 32), :], start, cs)
            up = 7.0 / high
            down = high * (-1.0 / 7.0)
            for q in range(4):
                rows = pl.ds(32 * q, 32)
                at = pl.ds(pl.multiple_of(start + 32 * q, 32), 32)
                w = w_ref[at, cs].astype(F32)
                s = sine_part(w * wide[0, rows, :] * up)
                full = w + s * down * wide[1, rows, :]
                acc[0, rows, cs] += full
                acc[1, rows, cs] += full * wide[2, rows, :]
                acc[2, rows, cs] += full * wide[3, rows, :]
                q_ref[at, cs] = (full * wide[4, rows, :]).astype(BF16)
        return carry

    lax.fori_loop(0, 8, block, 0)
    m_ref[...] = (acc[...] * (1.0 / math.sqrt(32.0))).astype(BF16)


def first_pick(weight, vectors):
    return pl.pallas_call(
        first_body,
        grid=(8,),
        in_specs=[
            pl.BlockSpec((1024, HALF), lambda h: (h, 0)),
            pl.BlockSpec((8, 8, 128), lambda h: (h, 0, 0)),
        ],
        out_specs=[
            pl.BlockSpec((1024, HALF), lambda h: (h, 0)),
            pl.BlockSpec((3, HEAD, HALF), lambda h: (0, h, 0)),
        ],
        out_shape=[
            jax.ShapeDtypeStruct((D, HALF), BF16),
            jax.ShapeDtypeStruct((3, KV, HALF), BF16),
        ],
        scratch_shapes=[pltpu.VMEM((3, HEAD, HALF), F32), pltpu.VMEM((5, GROUP, 128), F32)],
        name="first_pick",
    )(weight, vectors)


def deltas_body(w_ref, v_ref, d_ref, wide):
    def block(r, carry):
        spread_rows(v_ref[r], 8, wide)
        start = r * GROUP
        for p in range(PICKS):
            for c in range(4):
                cs = pl.ds(c * 128, 128)
                high = spacing_of(w_ref, lambda q: wide[p, pl.ds(32 * q, 32), :], start, cs)
                up = 7.0 / high
                down = high * (-1.0 / 7.0)
                for q in range(4):
                    rows = pl.ds(32 * q, 32)
                    at = pl.ds(pl.multiple_of(start + 32 * q, 32), 32)
                    w = w_ref[at, cs].astype(F32)
                    s = sine_part(w * wide[p, rows, :] * up)
                    d_ref[p, at, cs] = (s * down * wide[PICKS + p, rows, :]).astype(BF16)
        return carry

    lax.fori_loop(0, 8, block, 0)


def deltas(weight, vectors):
    return pl.pallas_call(
        deltas_body,
        grid=(8,),
        in_specs=[
            pl.BlockSpec((1024, HALF), lambda h: (h, 0)),
            pl.BlockSpec((8, 8, 128), lambda h: (h, 0, 0)),
        ],
        out_specs=pl.BlockSpec((PICKS, 1024, HALF), lambda h: (0, h, 0)),
        out_shape=jax.ShapeDtypeStruct((PICKS, D, HALF), BF16),
        scratch_shapes=[pltpu.VMEM((8, GROUP, 128), F32)],
        name="deltas",
    )(weight, vectors)


def nothing(weight):
    return pl.pallas_call(
        lambda w_ref, d_ref: None,
        in_specs=[pl.BlockSpec(memory_space=pl.ANY)],
        out_specs=pl.BlockSpec(memory_space=pl.ANY),
        out_shape=jax.ShapeDtypeStruct((PICKS, D, HALF), BF16),
        name="nothing",
    )(weight)


def losses_body(s_ref, d_ref, o_ref, acc):
    @pl.when(pl.program_id(0) == 0)
    def _():
        acc[...] = jnp.zeros_like(acc)

    for p in range(PICKS):
        acc[p] += jnp.dot(s_ref[...], d_ref[p], preferred_element_type=F32)

    @pl.when(pl.program_id(0) == pl.num_programs(0) - 1)
    def _():
        rows = []
        for p in range(PICKS):
            total = jnp.sum(jnp.square(acc[p]), axis=0, keepdims=True)
            rows.append(total[:, :128] + total[:, 128:256] + total[:, 256:384] + total[:, 384:])
        o_ref[...] = jnp.concatenate(rows + rows, axis=0)


def losses(stream, delta):
    depth = 512
    return pl.pallas_call(
        losses_body,
        grid=(D // depth,),
        in_specs=[
            pl.BlockSpec((128, depth), lambda k: (0, k)),
            pl.BlockSpec((PICKS, depth, HALF), lambda k: (0, k, 0)),
        ],
        out_specs=pl.BlockSpec((8, 128), lambda k: (0, 0)),
        out_shape=jax.ShapeDtypeStruct((8, 128), F32),
        scratch_shapes=[pltpu.VMEM((PICKS, 128, HALF), F32)],
        name="losses",
    )(stream, delta)


def reduce_body(x_ref, o_ref, slots, send_sem, recv_sem):
    dp, mp = lax.axis_size("dp"), lax.axis_size("mp")
    peers = dp * mp
    rank = lax.axis_index("dp") * mp + lax.axis_index("mp")
    barrier = pltpu.get_barrier_semaphore()

    def place(k):
        other = lax.rem(rank + k, peers)
        return {"dp": lax.div(other, mp), "mp": lax.rem(other, mp)}

    for k in range(1, peers):
        pl.semaphore_signal(barrier, inc=1, device_id=place(k), device_id_type=MESH)
    pl.semaphore_wait(barrier, peers - 1)
    slots[0] = x_ref[...]
    copies = []
    for k in range(1, peers):
        copy = pltpu.make_async_remote_copy(
            src_ref=x_ref,
            dst_ref=slots.at[k],
            send_sem=send_sem.at[k],
            recv_sem=recv_sem.at[k],
            device_id=place(k),
            device_id_type=MESH,
        )
        copy.start()
        copies.append(copy)
    for copy in copies:
        copy.wait()
    total = jnp.zeros_like(o_ref)
    for source in range(peers):
        total = total + slots[lax.rem(rank - source + peers, peers)]
    o_ref[...] = total


def reduce_all(part):
    return pl.pallas_call(
        reduce_body,
        in_specs=[pl.BlockSpec(memory_space=pltpu.VMEM)],
        out_specs=pl.BlockSpec(memory_space=pltpu.VMEM),
        out_shape=jax.ShapeDtypeStruct((8, 128), F32),
        scratch_shapes=[
            pltpu.VMEM((8, 8, 128), F32),
            pltpu.SemaphoreType.DMA((8,)),
            pltpu.SemaphoreType.DMA((8,)),
        ],
        compiler_params=pltpu.CompilerParams(collective_id=1, has_side_effects=True),
        name="reduce_all",
    )(part)


def chain_body(
    x_ref, q_ref, m_ref, v_ref, after_ref,
    out_ref, s_ref,
    full, fold, bulk, ahead, seen, near, mine,
    q_sem, m_sem, x_sem, near_send, near_recv, bulk_send, bulk_recv, save_sem, pair_send, pair_recv,
):
    sections = lax.axis_size("section")
    sec = lax.axis_index("section")
    half = lax.axis_index("mp")
    root = 1.0 / math.sqrt(sections)
    partner = {"mp": 1 - half}

    for i in range(3):
        @pl.when(sec <= i)
        def _():
            near[i] = jnp.zeros_like(near.at[i])

    barrier = pltpu.get_barrier_semaphore()
    pl.semaphore_signal(barrier, inc=1, device_id=partner, device_id_type=MESH)
    count = jnp.int32(1)
    for step in (1, 2, 3, 4):
        @pl.when(sec + step < sections)
        def _():
            pl.semaphore_signal(barrier, inc=1, device_id={"section": sec + step}, device_id_type=MESH)

        @pl.when(sec >= step)
        def _():
            pl.semaphore_signal(barrier, inc=1, device_id={"section": sec - step}, device_id_type=MESH)

        count = count + jnp.where(sec + step < sections, 1, 0) + jnp.where(sec >= step, 1, 0)
    pl.semaphore_wait(barrier, count)

    q_local = pltpu.make_async_copy(q_ref, full.at[half], q_sem.at[0])
    q_other = pltpu.make_async_remote_copy(
        src_ref=q_ref, dst_ref=full.at[half], send_sem=q_sem.at[1], recv_sem=q_sem.at[2],
        device_id=partner, device_id_type=MESH,
    )
    m_local = pltpu.make_async_copy(m_ref, fold.at[half], m_sem.at[0])
    m_other = pltpu.make_async_remote_copy(
        src_ref=m_ref, dst_ref=fold.at[half], send_sem=m_sem.at[1], recv_sem=m_sem.at[2],
        device_id=partner, device_id_type=MESH,
    )
    q_other.start()
    m_other.start()
    q_local.start()
    m_local.start()

    own_rows = pl.ds(pl.multiple_of(half * ROWS, ROWS), ROWS)
    x_copy = pltpu.make_async_copy(x_ref.at[:, own_rows, :], bulk, x_sem)

    @pl.when(sec < 4)
    def _():
        x_copy.start()
        x_copy.wait()

    q_local.wait()
    q_other.wait()
    m_local.wait()
    m_other.wait()

    def near_copy(i, w, target):
        return pltpu.make_async_remote_copy(
            src_ref=mine.at[w], dst_ref=near.at[i, w], send_sem=near_send.at[i, w],
            recv_sem=near_recv.at[i, w], device_id=target, device_id_type=MESH,
        )

    def bulk_copy(w, target):
        return pltpu.make_async_remote_copy(
            src_ref=ahead.at[w], dst_ref=bulk.at[w], send_sem=bulk_send.at[w],
            recv_sem=bulk_recv.at[w], device_id=target, device_id_type=MESH,
        )

    def tail_copies(w):
        own_cols = pl.ds(pl.multiple_of(half * HALF, HALF), HALF)
        other_cols = pl.ds(pl.multiple_of((1 - half) * HALF, HALF), HALF)
        return (
            pltpu.make_async_copy(mine.at[w, :, own_cols], out_ref.at[w, own_rows, :], save_sem.at[0, w]),
            pltpu.make_async_copy(seen.at[w], s_ref.at[w, own_rows, :], save_sem.at[1, w]),
        ), (
            pltpu.make_async_remote_copy(
                src_ref=mine.at[w, :, other_cols], dst_ref=out_ref.at[w, own_rows, :],
                send_sem=pair_send.at[0, w], recv_sem=pair_recv.at[0, w],
                device_id=partner, device_id_type=MESH,
            ),
            pltpu.make_async_remote_copy(
                src_ref=seen.at[w], dst_ref=s_ref.at[w, own_rows, :],
                send_sem=pair_send.at[1, w], recv_sem=pair_recv.at[1, w],
                device_id=partner, device_id_type=MESH,
            ),
        )

    def wave(w, carry):
        @pl.when(sec >= 4)
        def _():
            bulk_copy(w, {"section": sec}).wait_recv()

        def deep(k, sums):
            cs = pl.ds(pl.multiple_of(k * 1024, 1024), 1024)
            piece = bulk[w, :, cs]
            return (
                sums[0] + jnp.dot(piece, full[0, cs, :], preferred_element_type=F32),
                sums[1] + jnp.dot(piece, full[1, cs, :], preferred_element_type=F32),
            )

        zero = jnp.zeros((ROWS, HALF), F32)
        sums = lax.fori_loop(0, 8, deep, (zero, zero))
        for i in (2, 1, 0):
            @pl.when(sec >= i + 1)
            def _():
                near_copy(i, w, {"section": sec}).wait_recv()

            piece = near[i, w]
            sums = (
                sums[0] + jnp.dot(piece, fold[0, i], preferred_element_type=F32),
                sums[1] + jnp.dot(piece, fold[1, i], preferred_element_type=F32),
            )
        mine[w, :, :HALF] = sums[0].astype(BF16)
        mine[w, :, HALF:] = sums[1].astype(BF16)
        for i in range(3):
            @pl.when(sec + i + 1 < sections)
            def _():
                near_copy(i, w, {"section": sec + i + 1}).start()

        def assemble(c, carry):
            heads = pl.ds(pl.multiple_of(c * HEAD, HEAD), HEAD)
            y1 = near[0, w, :, heads].astype(F32) * root
            y2 = near[1, w, :, heads].astype(F32)
            y3 = near[2, w, :, heads].astype(F32)
            y0 = mine[w, :, heads].astype(F32) * root
            for r in range(8):
                cs = pl.ds(pl.multiple_of(c * 1024 + r * HEAD, HEAD), HEAD)
                now = (
                    v_ref[0:1, cs] * bulk[w, :, cs].astype(F32)
                    + v_ref[1:2, cs] * y3 + v_ref[2:3, cs] * y2 + y1
                )
                seen[w, :, cs] = now.astype(BF16)
                ahead[w, :, cs] = (v_ref[3:4, cs] * now + y0).astype(BF16)
            return carry

        lax.fori_loop(0, 8, assemble, 0)

        @pl.when(sec + 4 < sections)
        def _():
            bulk_copy(w, {"section": sec + 4}).start()

        local, remote = tail_copies(w)
        for copy in remote + local:
            copy.start()
        return carry

    lax.fori_loop(0, MICRO, wave, 0)

    def finish(w, carry):
        for i in range(3):
            @pl.when(sec + i + 1 < sections)
            def _():
                near_copy(i, w, {"section": sec + i + 1}).wait_send()

        @pl.when(sec + 4 < sections)
        def _():
            bulk_copy(w, {"section": sec + 4}).wait_send()

        local, remote = tail_copies(w)
        for copy in local:
            copy.wait()
        for copy in remote:
            copy.wait()
        return carry

    lax.fori_loop(0, MICRO, finish, 0)


def chain(inputs, quant, folds, vectors, after):
    anywhere = pl.BlockSpec(memory_space=pl.ANY)
    dma = pltpu.SemaphoreType.DMA
    return pl.pallas_call(
        chain_body,
        in_specs=[anywhere, anywhere, anywhere, pl.BlockSpec(memory_space=pltpu.VMEM), anywhere],
        out_specs=[anywhere, anywhere],
        out_shape=[
            jax.ShapeDtypeStruct((MICRO, 32, HALF), BF16),
            jax.ShapeDtypeStruct((MICRO, 32, D), BF16),
        ],
        scratch_shapes=[
            pltpu.VMEM((2, D, HALF), BF16),
            pltpu.VMEM((2, 3, KV, HALF), BF16),
            pltpu.VMEM((MICRO, ROWS, D), BF16),
            pltpu.VMEM((MICRO, ROWS, D), BF16),
            pltpu.VMEM((MICRO, ROWS, D), BF16),
            pltpu.VMEM((3, MICRO, ROWS, KV), BF16),
            pltpu.VMEM((MICRO, ROWS, KV), BF16),
            dma((3,)),
            dma((3,)),
            dma,
            dma((3, MICRO)),
            dma((3, MICRO)),
            dma((MICRO,)),
            dma((MICRO,)),
            dma((2, MICRO)),
            dma((2, MICRO)),
            dma((2, MICRO)),
        ],
        compiler_params=pltpu.CompilerParams(
            collective_id=0, has_side_effects=True, vmem_limit_bytes=60 * 1024 * 1024
        ),
        name="chain",
    )(inputs, quant, folds, vectors, after)


def from_behind(block, distance):
    sections = lax.axis_size("section")
    route = [(i - distance, i) for i in range(distance, sections)]
    moved = lax.ppermute(block, "section", route)
    return jnp.where(lax.axis_index("section") >= distance, moved, 1.0)


def local(inputs, value_weight, carry_gain, channel_bins, grid_picks):
    sec = lax.axis_index("section")
    weight = value_weight[0]
    own = carry_gain[0]
    g1 = from_behind(own, 1)
    g2 = from_behind(own, 2)
    g3 = from_behind(own, 3)
    g12 = g1 * g2
    g123 = g12 * g3
    exponent = grid_picks[0, :PICKS].astype(F32) / GRID
    scaling = jnp.exp2(exponent[:, None] * channel_bins[0].astype(F32)[None, :] / 4.0)
    inverse = 1.0 / scaling
    one = jnp.ones_like(g1)
    by_block = jnp.stack([scaling[0], inverse[0], g1, g12, g123, one, one, one])
    by_block = by_block.reshape(8, D // GROUP, GROUP).transpose(1, 0, 2)
    quant, folds = first_pick(weight, by_block)
    picks = jnp.concatenate([scaling, inverse]).reshape(8, D // GROUP, GROUP).transpose(1, 0, 2)
    weight, picks, quant, folds = lax.optimization_barrier((weight, picks, quant, folds))
    early_delta = lax.cond(sec >= LATE, lambda: deltas(weight, picks), lambda: nothing(weight))
    root = 1.0 / math.sqrt(lax.axis_size("section"))
    rows = jnp.stack([g123, g12 * root, g1 * root, own])
    quant_out, stream = chain(inputs, quant, folds, rows, early_delta)
    flat = stream.reshape(MICRO * 32, D)
    part = lax.cond(
        sec >= LATE,
        lambda: losses(flat, early_delta),
        lambda: losses(flat, deltas(weight, picks)),
    )
    total = reduce_all(part)
    entry_count = inputs.shape[0] * inputs.shape[1] * lax.axis_size("dp") * KV
    grid_loss = jnp.sum(total[:PICKS], axis=1) * (LOSS_UNIT / entry_count)
    return (quant_out[None], grid_loss[None])


def solution(mesh):
    placed = (
        P(None, "dp", None),
        P("section", None, "mp"),
        P("section", None),
        P("section", None),
        P("section", None),
    )
    return jax.shard_map(
        local,
        mesh=mesh,
        in_specs=placed,
        out_specs=(P("section", None, "dp", "mp"), P("section", None)),
        check_vma=False,
    )
```

```python
import functools
import math

import jax
import jax.numpy as jnp
from jax import lax
from jax.experimental import pallas as pl
from jax.experimental.pallas import tpu as pltpu
from jax.sharding import PartitionSpec as P

D = 8192
KV = 1024
HALF = 512
HEAD = 128
GROUP = 128
GRID = 20
PICKS = 4
MICRO = 4
ROWS = 16
BEFORE = (10, 15, 20, 25)

EPS = 1e-06
LOSS_UNIT = 1000.0
MESH = pl.DeviceIdType.MESH
SINE = (
    0.9999996039221354,
    -6.579691570017649,
    12.98643600013728,
    -12.188101534445755,
    6.558042246424786,
    -1.953032018015784,
)
F32 = jnp.float32
BF16 = jnp.bfloat16


def sine_part(levels):
    r = levels - jnp.round(levels)
    z = r * r
    acc = jnp.full_like(z, SINE[-1])
    for c in SINE[-2::-1]:
        acc = acc * z + c
    return acc * r


def high_of(w_ref, wide, r, start, cs):
    high = None
    for q in range(4):
        part = w_ref[pl.ds(pl.multiple_of(start + 32 * q, 32), 32), cs].astype(F32)
        part = jnp.abs(part * wide[r, pl.ds(32 * q, 32), :])
        part = jnp.max(part, axis=0, keepdims=True)
        high = part if high is None else jnp.maximum(high, part)
    return high + EPS


def scales_of(bins, pick, wide, back):
    exponent = jnp.full(bins.shape, pick, jnp.int32).astype(F32) / GRID
    scaling = jnp.exp2(exponent * bins.astype(F32) / 4.0)
    columns, inverse = scaling.T, (1.0 / scaling).T
    for r in range(8):
        wide[r] = jnp.broadcast_to(columns[:, r : r + 1], (GROUP, 128))
        back[r] = jnp.broadcast_to(inverse[:, r : r + 1], (GROUP, 128))


def rounding_part(w, scale, back, up, down):
    return sine_part(w * scale * up) * down * back


def first_body(picks_ref, bins_ref, g_ref, w_ref, x_ref, q_ref, m_ref, a_ref, wide, back, left, acc):
    head = pl.program_id(0)
    scales_of(bins_ref[...], picks_ref[0, 0], wide, back)
    eye = lax.broadcasted_iota(jnp.int32, (HEAD, HEAD), 0) == lax.broadcasted_iota(jnp.int32, (HEAD, HEAD), 1)
    for r in range(8):
        cs = pl.ds(r * HEAD, HEAD)
        row = jnp.ones((1, HEAD), F32)
        for i, gain in enumerate((row, g_ref[2, r : r + 1, :], g_ref[1, r : r + 1, :])):
            left[i * HEAD : (i + 1) * HEAD, cs] = jnp.where(eye, gain, 0.0).astype(BF16)
        for w in range(MICRO):
            left[384 + w * 32 : 416 + w * 32, cs] = (
                x_ref[w, :, cs].astype(F32) * g_ref[0, r : r + 1, :]
            ).astype(BF16)

    def block(r, carry):
        start = r * GROUP
        for c in range(4):
            cs = pl.ds(c * 128, 128)
            high = high_of(w_ref, wide, r, start, cs)
            up = 7.0 / high
            down = high * (-1.0 / 7.0)
            for q in range(4):
                rows = pl.ds(32 * q, 32)
                at = pl.ds(pl.multiple_of(start + 32 * q, 32), 32)
                w = w_ref[at, cs].astype(F32)
                q_ref[at, cs] = (w + rounding_part(w, wide[r, rows, :], back[r, rows, :], up, down)).astype(BF16)
        return carry

    lax.fori_loop(0, 8, block, 0)
    product = jnp.dot(left[...], q_ref[...], preferred_element_type=F32)
    for i in range(3):
        m_ref[i] = (product[i * HEAD : (i + 1) * HEAD] * (1.0 / math.sqrt(32.0))).astype(BF16)

    @pl.when(head == 0)
    def _():
        acc[...] = product[384:]

    @pl.when(head > 0)
    def _():
        acc[...] += product[384:]

    @pl.when(head == 7)
    def _():
        for w in range(MICRO):
            a_ref[w] = acc[w * 32 : w * 32 + 32]


def first_pick(picks, bins, gains, weight, inputs):
    return pl.pallas_call(
        first_body,
        grid=(8,),
        in_specs=[
            pl.BlockSpec(memory_space=pltpu.SMEM),
            pl.BlockSpec((8, 128), lambda h: (h, 0)),
            pl.BlockSpec((4, 8, 128), lambda h: (0, h, 0)),
            pl.BlockSpec((1024, HALF), lambda h: (h, 0)),
            pl.BlockSpec((MICRO, 32, 1024), lambda h: (0, 0, h)),
        ],
        out_specs=[
            pl.BlockSpec((1024, HALF), lambda h: (h, 0)),
            pl.BlockSpec((3, HEAD, HALF), lambda h: (0, h, 0)),
            pl.BlockSpec((MICRO, 32, HALF), lambda h: (0, 0, 0)),
        ],
        out_shape=[
            jax.ShapeDtypeStruct((D, HALF), BF16),
            jax.ShapeDtypeStruct((3, KV, HALF), BF16),
            jax.ShapeDtypeStruct((MICRO, 32, HALF), F32),
        ],
        scratch_shapes=[
            pltpu.VMEM((8, GROUP, 128), F32),
            pltpu.VMEM((8, GROUP, 128), F32),
            pltpu.VMEM((512, 1024), BF16),
            pltpu.VMEM((128, HALF), F32),
        ],
        name="first_pick",
    )(picks, bins, gains, weight, inputs)


def picks_before(sec):
    return sum(jnp.where(sec >= least, 1, 0) for least in BEFORE)


def deltas_body(later, picks_ref, bins_ref, w_ref, old_ref, after_ref, d_ref, held, made, wide, back, w_sem, d_sem):
    split = picks_before(lax.axis_index("section"))
    low, count = (split, (PICKS - split) * 8) if later else (0, split * 8)

    def fetch(h):
        at = pl.ds(pl.multiple_of(h * 1024, 1024), 1024)
        return pltpu.make_async_copy(w_ref.at[at, :], held.at[at, :], w_sem.at[h])

    def put(t):
        at = pl.ds(pl.multiple_of(lax.rem(t, 8) * 1024, 1024), 1024)
        slot = lax.rem(t, 2)
        return pltpu.make_async_copy(made.at[slot], d_ref.at[low + lax.div(t, 8), at, :], d_sem.at[slot])

    @pl.when(count > 0)
    def _():
        for h in range(8):
            fetch(h).start()

    def step(t, carry):
        h = lax.rem(t, 8)
        slot = lax.rem(t, 2)

        @pl.when(t < 8)
        def _():
            fetch(h).wait()

        @pl.when(t >= 2)
        def _():
            put(t - 2).wait()

        scales_of(bins_ref[pl.ds(pl.multiple_of(h * 8, 8), 8), :], picks_ref[0, low + lax.div(t, 8)], wide, back)

        def block(r, carry):
            start = h * 1024 + r * GROUP
            for c in range(4):
                cs = pl.ds(c * 128, 128)
                high = high_of(held, wide, r, start, cs)
                up = 7.0 / high
                down = high * (-1.0 / 7.0)
                for q in range(4):
                    rows = pl.ds(32 * q, 32)
                    w = held[pl.ds(pl.multiple_of(start + 32 * q, 32), 32), cs].astype(F32)
                    made[slot, pl.ds(pl.multiple_of(r * GROUP + 32 * q, 32), 32), cs] = rounding_part(
                        w, wide[r, rows, :], back[r, rows, :], up, down
                    ).astype(BF16)
            return carry

        lax.fori_loop(0, 8, block, 0)
        put(t).start()
        return carry

    lax.fori_loop(0, count, step, 0)

    @pl.when(count > 0)
    def _():
        put(count - 2).wait()
        put(count - 1).wait()


def deltas(later, picks, bins, weight, old, after):
    anywhere = pl.BlockSpec(memory_space=pl.ANY)
    return pl.pallas_call(
        functools.partial(deltas_body, later),
        in_specs=[
            pl.BlockSpec(memory_space=pltpu.SMEM),
            pl.BlockSpec(memory_space=pltpu.VMEM),
            anywhere,
            anywhere,
            anywhere,
        ],
        out_specs=anywhere,
        out_shape=jax.ShapeDtypeStruct((PICKS, D, HALF), BF16),
        input_output_aliases={3: 0} if later else {},
        scratch_shapes=[
            pltpu.VMEM((D, HALF), BF16),
            pltpu.VMEM((2, 1024, HALF), BF16),
            pltpu.VMEM((8, GROUP, 128), F32),
            pltpu.VMEM((8, GROUP, 128), F32),
            pltpu.SemaphoreType.DMA((8,)),
            pltpu.SemaphoreType.DMA((2,)),
        ],
        name="deltas_later" if later else "deltas_before",
    )(picks, bins, weight, old, after)


def losses_body(s_ref, d_ref, o_ref, acc):
    part = pl.program_id(1)
    product = jnp.dot(s_ref[part], d_ref[0], preferred_element_type=F32)

    @pl.when(part == 0)
    def _():
        acc[...] = product

    @pl.when(part > 0)
    def _():
        acc[...] += product

    @pl.when(part == pl.num_programs(1) - 1)
    def _():
        total = jnp.sum(jnp.square(acc[...]), axis=0, keepdims=True)
        total = total[:, :128] + total[:, 128:256] + total[:, 256:384] + total[:, 384:]
        o_ref[pl.ds(pl.program_id(0), 1), :] = total


def losses(stream, delta):
    depth = 2048
    parts = D // depth
    return pl.pallas_call(
        losses_body,
        grid=(PICKS, parts),
        in_specs=[
            pl.BlockSpec((parts, 128, depth), lambda p, k: (0, 0, 0)),
            pl.BlockSpec((1, depth, HALF), lambda p, k: (p, k, 0)),
        ],
        out_specs=pl.BlockSpec((8, 128), lambda p, k: (0, 0)),
        out_shape=jax.ShapeDtypeStruct((8, 128), F32),
        scratch_shapes=[pltpu.VMEM((128, HALF), F32)],
        name="losses",
    )(stream, delta)


def gains_body(own_ref, o_ref, got, send_sem, recv_sem):
    sections = lax.axis_size("section")
    sec = lax.axis_index("section")
    for i in range(3):
        @pl.when(sec <= i)
        def _():
            got[i] = jnp.ones_like(own_ref)

    barrier = pltpu.get_barrier_semaphore()
    count = jnp.int32(0)
    for step in (1, 2, 3):
        @pl.when(sec + step < sections)
        def _():
            pl.semaphore_signal(barrier, inc=1, device_id={"section": sec + step}, device_id_type=MESH)

        @pl.when(sec >= step)
        def _():
            pl.semaphore_signal(barrier, inc=1, device_id={"section": sec - step}, device_id_type=MESH)

        count = count + jnp.where(sec + step < sections, 1, 0) + jnp.where(sec >= step, 1, 0)
    pl.semaphore_wait(barrier, count)

    def copy(i):
        return pltpu.make_async_remote_copy(
            src_ref=own_ref, dst_ref=got.at[i], send_sem=send_sem.at[i], recv_sem=recv_sem.at[i],
            device_id={"section": jnp.minimum(sec + i + 1, sections - 1)}, device_id_type=MESH,
        )

    for i in range(3):
        @pl.when(sec + i + 1 < sections)
        def _():
            copy(i).start()

    for i in range(3):
        @pl.when(sec > i)
        def _():
            copy(i).wait_recv()

    g1 = got[0]
    g12 = g1 * got[1]
    o_ref[0] = g12 * got[2]
    o_ref[1] = g12
    o_ref[2] = g1
    o_ref[3] = own_ref[...]
    for i in range(3):
        @pl.when(sec + i + 1 < sections)
        def _():
            copy(i).wait_send()


def gains_of(own):
    return pl.pallas_call(
        gains_body,
        in_specs=[pl.BlockSpec(memory_space=pltpu.VMEM)],
        out_specs=pl.BlockSpec(memory_space=pltpu.VMEM),
        out_shape=jax.ShapeDtypeStruct((4, D // 128, 128), F32),
        scratch_shapes=[
            pltpu.VMEM((3, D // 128, 128), F32),
            pltpu.SemaphoreType.DMA((3,)),
            pltpu.SemaphoreType.DMA((3,)),
        ],
        compiler_params=pltpu.CompilerParams(collective_id=2, has_side_effects=True),
        name="gains",
    )(own)


def reduce_body(x_ref, o_ref, slots, send_sem, recv_sem):
    dp, mp = lax.axis_size("dp"), lax.axis_size("mp")
    peers = dp * mp
    rank = lax.axis_index("dp") * mp + lax.axis_index("mp")
    barrier = pltpu.get_barrier_semaphore()

    def place(k):
        other = lax.rem(rank + k, peers)
        return {"dp": lax.div(other, mp), "mp": lax.rem(other, mp)}

    for k in range(1, peers):
        pl.semaphore_signal(barrier, inc=1, device_id=place(k), device_id_type=MESH)
    pl.semaphore_wait(barrier, peers - 1)
    slots[0] = x_ref[...]
    copies = []
    for k in range(1, peers):
        copy = pltpu.make_async_remote_copy(
            src_ref=x_ref,
            dst_ref=slots.at[k],
            send_sem=send_sem.at[k],
            recv_sem=recv_sem.at[k],
            device_id=place(k),
            device_id_type=MESH,
        )
        copy.start()
        copies.append(copy)
    for copy in copies:
        copy.wait()
    total = jnp.zeros_like(o_ref)
    for source in range(peers):
        total = total + slots[lax.rem(rank - source + peers, peers)]
    o_ref[...] = total


def reduce_all(part):
    return pl.pallas_call(
        reduce_body,
        in_specs=[pl.BlockSpec(memory_space=pltpu.VMEM)],
        out_specs=pl.BlockSpec(memory_space=pltpu.VMEM),
        out_shape=jax.ShapeDtypeStruct((8, 128), F32),
        scratch_shapes=[
            pltpu.VMEM((8, 8, 128), F32),
            pltpu.SemaphoreType.DMA((8,)),
            pltpu.SemaphoreType.DMA((8,)),
        ],
        compiler_params=pltpu.CompilerParams(collective_id=1, has_side_effects=True),
        name="reduce_all",
    )(part)


def chain_body(
    x_ref, q_ref, m_ref, a_ref, v_ref, after_ref,
    out_ref, s_ref,
    full, fold, start, bulk, ahead, seen, near, mine,
    q_sem, m_sem, a_sem, x_sem, near_send, near_recv, bulk_send, bulk_recv, save_sem, pair_send, pair_recv,
):
    sections = lax.axis_size("section")
    sec = lax.axis_index("section")
    half = lax.axis_index("mp")
    root = 1.0 / math.sqrt(sections)
    partner = {"mp": 1 - half}

    for i in range(3):
        @pl.when(sec <= i)
        def _():
            near[i] = jnp.zeros_like(near.at[i])

    barrier = pltpu.get_barrier_semaphore()
    pl.semaphore_signal(barrier, inc=1, device_id=partner, device_id_type=MESH)
    count = jnp.int32(1)
    for step in (1, 2, 3, 4):
        @pl.when(sec + step < sections)
        def _():
            pl.semaphore_signal(barrier, inc=1, device_id={"section": sec + step}, device_id_type=MESH)

        @pl.when(sec >= step)
        def _():
            pl.semaphore_signal(barrier, inc=1, device_id={"section": sec - step}, device_id_type=MESH)

        count = count + jnp.where(sec + step < sections, 1, 0) + jnp.where(sec >= step, 1, 0)
    pl.semaphore_wait(barrier, count)

    q_local = pltpu.make_async_copy(q_ref, full.at[half], q_sem.at[0])
    q_other = pltpu.make_async_remote_copy(
        src_ref=q_ref, dst_ref=full.at[half], send_sem=q_sem.at[1], recv_sem=q_sem.at[2],
        device_id=partner, device_id_type=MESH,
    )
    m_local = pltpu.make_async_copy(m_ref, fold.at[half], m_sem.at[0])
    m_other = pltpu.make_async_remote_copy(
        src_ref=m_ref, dst_ref=fold.at[half], send_sem=m_sem.at[1], recv_sem=m_sem.at[2],
        device_id=partner, device_id_type=MESH,
    )
    own_rows = pl.ds(pl.multiple_of(half * ROWS, ROWS), ROWS)
    other_rows = pl.ds(pl.multiple_of((1 - half) * ROWS, ROWS), ROWS)
    a_local = pltpu.make_async_copy(a_ref.at[:, own_rows, :], start.at[half], a_sem.at[0])
    a_other = pltpu.make_async_remote_copy(
        src_ref=a_ref.at[:, other_rows, :], dst_ref=start.at[half], send_sem=a_sem.at[1], recv_sem=a_sem.at[2],
        device_id=partner, device_id_type=MESH,
    )
    x_copy = pltpu.make_async_copy(x_ref.at[:, own_rows, :], bulk, x_sem)
    a_other.start()
    m_other.start()
    a_local.start()
    m_local.start()

    @pl.when(sec < 4)
    def _():
        x_copy.start()
        x_copy.wait()

    @pl.when(sec >= 4)
    def _():
        q_other.start()
        q_local.start()

    a_local.wait()
    a_other.wait()

    @pl.when(sec >= 1)
    def _():
        m_local.wait()
        m_other.wait()

    @pl.when(sec >= 4)
    def _():
        q_local.wait()
        q_other.wait()

    def near_copy(i, w, target):
        return pltpu.make_async_remote_copy(
            src_ref=mine.at[w], dst_ref=near.at[i, w], send_sem=near_send.at[i, w],
            recv_sem=near_recv.at[i, w], device_id=target, device_id_type=MESH,
        )

    def bulk_copy(w, target):
        return pltpu.make_async_remote_copy(
            src_ref=ahead.at[w], dst_ref=bulk.at[w], send_sem=bulk_send.at[w],
            recv_sem=bulk_recv.at[w], device_id=target, device_id_type=MESH,
        )

    def tail_copies(w):
        own_cols = pl.ds(pl.multiple_of(half * HALF, HALF), HALF)
        other_cols = pl.ds(pl.multiple_of((1 - half) * HALF, HALF), HALF)
        return (
            pltpu.make_async_copy(mine.at[w, :, own_cols], out_ref.at[w, own_rows, :], save_sem.at[0, w]),
            pltpu.make_async_copy(seen.at[w], s_ref.at[:, w, own_rows, :], save_sem.at[1, w]),
        ), (
            pltpu.make_async_remote_copy(
                src_ref=mine.at[w, :, other_cols], dst_ref=out_ref.at[w, own_rows, :],
                send_sem=pair_send.at[0, w], recv_sem=pair_recv.at[0, w],
                device_id=partner, device_id_type=MESH,
            ),
            pltpu.make_async_remote_copy(
                src_ref=seen.at[w], dst_ref=s_ref.at[:, w, own_rows, :],
                send_sem=pair_send.at[1, w], recv_sem=pair_recv.at[1, w],
                device_id=partner, device_id_type=MESH,
            ),
        )

    def wave(w, carry):
        def deep(k, sums):
            cs = pl.ds(pl.multiple_of(k * 1024, 1024), 1024)
            piece = jnp.concatenate([
                (
                    bulk[w, :, pl.ds(pl.multiple_of(k * 1024 + r * HEAD, HEAD), HEAD)].astype(F32)
                    * v_ref[0, pl.ds(k * 8 + r, 1), :]
                ).astype(BF16)
                for r in range(8)
            ], axis=1)
            return (
                sums[0] + jnp.dot(piece, full[0, cs, :], preferred_element_type=F32),
                sums[1] + jnp.dot(piece, full[1, cs, :], preferred_element_type=F32),
            )

        def from_bulk():
            bulk_copy(w, {"section": sec}).wait_recv()
            zero = jnp.zeros((ROWS, HALF), F32)
            return lax.fori_loop(0, 8, deep, (zero, zero))

        def from_start():
            return (start[0, w], start[1, w])

        sums = lax.cond(sec >= 4, from_bulk, from_start)
        for i in (2, 1, 0):
            def more(sums, i=i):
                near_copy(i, w, {"section": sec}).wait_recv()
                piece = near[i, w]
                return (
                    sums[0] + jnp.dot(piece, fold[0, i], preferred_element_type=F32),
                    sums[1] + jnp.dot(piece, fold[1, i], preferred_element_type=F32),
                )

            sums = lax.cond(sec > i, more, lambda sums: sums, sums)
        mine[w, :, :HALF] = sums[0].astype(BF16)
        mine[w, :, HALF:] = sums[1].astype(BF16)
        for i in range(3):
            @pl.when(sec + i + 1 < sections)
            def _():
                near_copy(i, w, {"section": sec + i + 1}).start()

        def assemble(c, carry):
            heads = pl.ds(pl.multiple_of(c * HEAD, HEAD), HEAD)
            y1 = near[0, w, :, heads].astype(F32) * root
            y2 = near[1, w, :, heads].astype(F32) * root
            y3 = near[2, w, :, heads].astype(F32) * root
            y0 = mine[w, :, heads].astype(F32) * root
            for r in range(8):
                cs = pl.ds(pl.multiple_of(c * 1024 + r * HEAD, HEAD), HEAD)
                row = pl.ds(c * 8 + r, 1)
                now = v_ref[0, row, :] * bulk[w, :, cs].astype(F32) + v_ref[1, row, :] * y3 + v_ref[2, row, :] * y2 + y1
                spot = pl.ds(pl.multiple_of(lax.rem(c, 2) * 1024 + r * HEAD, HEAD), HEAD)
                seen[w, lax.div(c, 2), :, spot] = now.astype(BF16)
                ahead[w, :, cs] = (v_ref[3, row, :] * now + y0).astype(BF16)
            return carry

        lax.fori_loop(0, 8, assemble, 0)

        @pl.when(sec + 4 < sections)
        def _():
            bulk_copy(w, {"section": sec + 4}).start()

        local, remote = tail_copies(w)
        for copy in remote + local:
            copy.start()
        return carry

    lax.fori_loop(0, MICRO, wave, 0)

    def finish(w, carry):
        for i in range(3):
            @pl.when(sec + i + 1 < sections)
            def _():
                near_copy(i, w, {"section": sec + i + 1}).wait_send()

        @pl.when(sec + 4 < sections)
        def _():
            bulk_copy(w, {"section": sec + 4}).wait_send()

        local, remote = tail_copies(w)
        for copy in local:
            copy.wait()
        for copy in remote:
            copy.wait()
        return carry

    lax.fori_loop(0, MICRO, finish, 0)

    @pl.when(sec < 1)
    def _():
        m_local.wait()
        m_other.wait()


def chain(inputs, quant, folds, first, vectors, after):
    anywhere = pl.BlockSpec(memory_space=pl.ANY)
    dma = pltpu.SemaphoreType.DMA
    return pl.pallas_call(
        chain_body,
        in_specs=[anywhere, anywhere, anywhere, anywhere, pl.BlockSpec(memory_space=pltpu.VMEM), anywhere],
        out_specs=[anywhere, anywhere],
        out_shape=[
            jax.ShapeDtypeStruct((MICRO, 32, HALF), BF16),
            jax.ShapeDtypeStruct((4, MICRO, 32, D // 4), BF16),
        ],
        scratch_shapes=[
            pltpu.VMEM((2, D, HALF), BF16),
            pltpu.VMEM((2, 3, KV, HALF), BF16),
            pltpu.VMEM((2, MICRO, ROWS, HALF), F32),
            pltpu.VMEM((MICRO, ROWS, D), BF16),
            pltpu.VMEM((MICRO, ROWS, D), BF16),
            pltpu.VMEM((MICRO, 4, ROWS, D // 4), BF16),
            pltpu.VMEM((3, MICRO, ROWS, KV), BF16),
            pltpu.VMEM((MICRO, ROWS, KV), BF16),
            dma((3,)),
            dma((3,)),
            dma((3,)),
            dma,
            dma((3, MICRO)),
            dma((3, MICRO)),
            dma((MICRO,)),
            dma((MICRO,)),
            dma((2, MICRO)),
            dma((2, MICRO)),
            dma((2, MICRO)),
        ],
        compiler_params=pltpu.CompilerParams(
            collective_id=0, has_side_effects=True, vmem_limit_bytes=60 * 1024 * 1024
        ),
        name="chain",
    )(inputs, quant, folds, first, vectors, after)


def local(inputs, value_weight, carry_gain, channel_bins, grid_picks):
    weight = value_weight[0]
    bins = channel_bins.reshape(D // 128, 128)
    gains = gains_of(carry_gain.reshape(D // 128, 128))
    quant, folds, first = first_pick(grid_picks, bins, gains, weight, inputs)
    delta = deltas(False, grid_picks, bins, weight, folds, quant)
    quant_out, stream = chain(inputs, quant, folds, first, gains, delta)
    delta = deltas(True, grid_picks, bins, weight, delta, stream)
    part = losses(stream.reshape(4, MICRO * 32, D // 4), delta)
    total = reduce_all(part)
    entry_count = inputs.shape[0] * inputs.shape[1] * lax.axis_size("dp") * KV
    grid_loss = jnp.sum(total[:PICKS], axis=1) * (LOSS_UNIT / entry_count)
    return (quant_out[None], grid_loss[None])


def solution(mesh):
    placed = (
        P(None, "dp", None),
        P("section", None, "mp"),
        P("section", None),
        P("section", None),
        P("section", None),
    )
    return jax.shard_map(
        local,
        mesh=mesh,
        in_specs=placed,
        out_specs=(P("section", None, "dp", "mp"), P("section", None)),
        check_vma=False,
    )
```

```python
import functools
import math

import jax
import jax.numpy as jnp
from jax import lax
from jax.experimental import pallas as pl
from jax.experimental.pallas import tpu as pltpu
from jax.sharding import PartitionSpec as P

D = 8192
KV = 1024
HALF = 512
HEAD = 128
GROUP = 128
GRID = 20
PICKS = 4
MICRO = 4
ROWS = 16
BEFORE = (9, 14, 20, 25)

EPS = 1e-06
LOSS_UNIT = 1000.0
MESH = pl.DeviceIdType.MESH
SINE = (
    0.9999996039221354,
    -6.579691570017649,
    12.98643600013728,
    -12.188101534445755,
    6.558042246424786,
    -1.953032018015784,
)
F32 = jnp.float32
BF16 = jnp.bfloat16


def sine_part(levels):
    r = levels - jnp.round(levels)
    z = r * r
    acc = jnp.full_like(z, SINE[-1])
    for c in SINE[-2::-1]:
        acc = acc * z + c
    return acc * r


def high_of(w_ref, wide, r, cs):
    high = None
    for q in range(4):
        part = w_ref[r * GROUP + 32 * q : r * GROUP + 32 * q + 32, cs].astype(F32)
        part = jnp.abs(part * wide[r, 32 * q : 32 * q + 32, :])
        part = jnp.max(part, axis=0, keepdims=True)
        high = part if high is None else jnp.maximum(high, part)
    return high + EPS


def quantized(w_ref, wide, back, r, put):
    for c in range(4):
        cs = slice(c * 128, c * 128 + 128)
        high = high_of(w_ref, wide, r, cs)
        up = 7.0 / high
        down = high * (-1.0 / 7.0)
        for q in range(4):
            rows = slice(32 * q, 32 * q + 32)
            at = slice(r * GROUP + 32 * q, r * GROUP + 32 * q + 32)
            w = w_ref[at, cs].astype(F32)
            put(at, cs, rounding_part(w, wide[r, rows, :], back[r, rows, :], up, down).astype(BF16))


def scales_of(bins, pick, wide, back):
    exponent = jnp.full(bins.shape, pick, jnp.int32).astype(F32) / GRID
    scaling = jnp.exp2(exponent * bins.astype(F32) / 4.0)
    columns, inverse = scaling.T, (1.0 / scaling).T
    for r in range(8):
        wide[r] = jnp.broadcast_to(columns[:, r : r + 1], (GROUP, 128))
        back[r] = jnp.broadcast_to(inverse[:, r : r + 1], (GROUP, 128))


def rounding_part(w, scale, back, up, down):
    return sine_part(w * scale * up) * down * back


def first_body(
    picks_ref, bins_ref, g_ref, w_ref, x_ref,
    q_ref, m_ref, a_ref,
    wide, back, near_gain, far_gain, left, acc, made, folds, first,
    q_sem, m_sem, a_sem,
):
    head = pl.program_id(0)
    half = lax.axis_index("mp")
    partner = {"mp": 1 - half}

    def pieces(h):
        at = pl.ds(pl.multiple_of(h * 1024, 1024), 1024)
        src = made.at[h]
        rows = pl.ds(pl.multiple_of(h * HEAD, HEAD), HEAD)
        return (
            pltpu.make_async_copy(src, q_ref.at[half, at, :], q_sem.at[0, h]),
            pltpu.make_async_copy(folds.at[:, rows, :], m_ref.at[half, :, rows, :], m_sem.at[0, h]),
            pltpu.make_async_remote_copy(
                src_ref=folds.at[:, rows, :], dst_ref=m_ref.at[half, :, rows, :],
                send_sem=m_sem.at[1, h], recv_sem=m_sem.at[2, h], device_id=partner, device_id_type=MESH,
            ),
            pltpu.make_async_remote_copy(
                src_ref=src, dst_ref=q_ref.at[half, at, :],
                send_sem=q_sem.at[1, h], recv_sem=q_sem.at[2, h], device_id=partner, device_id_type=MESH,
            ),
        )

    @pl.when(head == 0)
    def _():
        barrier = pltpu.get_barrier_semaphore()
        pl.semaphore_signal(barrier, inc=1, device_id=partner, device_id_type=MESH)
        pl.semaphore_wait(barrier, 1)
        acc[...] = jnp.zeros_like(acc)

    scales_of(bins_ref[...], picks_ref[0, 0], wide, back)
    near_columns, far_columns = g_ref[2].T, g_ref[1].T
    for r in range(8):
        near_gain[r] = jnp.broadcast_to(near_columns[:, r : r + 1], (GROUP, 128))
        far_gain[r] = jnp.broadcast_to(far_columns[:, r : r + 1], (GROUP, 128))
        cs = slice(r * HEAD, r * HEAD + HEAD)
        for w in range(MICRO):
            left[w * 32 : w * 32 + 32, cs] = (x_ref[w, :, cs].astype(F32) * g_ref[0, r : r + 1, :]).astype(BF16)

    head_rows = pl.multiple_of(head * HEAD, HEAD)
    root = 1.0 / math.sqrt(32.0)
    for c in range(4):
        cs = slice(c * 128, c * 128 + 128)
        highs = [high_of(w_ref, wide, r, cs) for r in range(8)]
        ups = [7.0 / high for high in highs]
        downs = [high * (-1.0 / 7.0) for high in highs]
        for q in range(4):
            rows = slice(32 * q, 32 * q + 32)
            sums = None
            for r in range(8):
                at = slice(r * GROUP + 32 * q, r * GROUP + 32 * q + 32)
                w = w_ref[at, cs].astype(F32)
                value = w + rounding_part(w, wide[r, rows, :], back[r, rows, :], ups[r], downs[r])
                made[head, at, cs] = value.astype(BF16)
                terms = (value, value * near_gain[r, rows, :], value * far_gain[r, rows, :])
                sums = terms if sums is None else tuple(x + y for x, y in zip(sums, terms))
            for i in range(3):
                folds[i, pl.ds(head_rows + 32 * q, 32), cs] = (sums[i] * root).astype(BF16)
        if c % 2:
            half_cols = slice(c * 128 - 128, c * 128 + 128)
            acc[:, half_cols] += jnp.dot(left[...], made[head, :, half_cols], preferred_element_type=F32)
    for copy in pieces(head):
        copy.start()

    @pl.when(head == 7)
    def _():
        for side in range(2):
            for w in range(MICRO):
                at = w * 32 + side * ROWS
                first[side, w] = acc[at : at + ROWS, :]
        local = pltpu.make_async_copy(first.at[half], a_ref.at[half], a_sem.at[0])
        other = pltpu.make_async_remote_copy(
            src_ref=first.at[1 - half], dst_ref=a_ref.at[half], send_sem=a_sem.at[1], recv_sem=a_sem.at[2],
            device_id=partner, device_id_type=MESH,
        )
        other.start()
        local.start()

        def finish(h, carry):
            for copy in pieces(h):
                copy.wait()
            return carry

        lax.fori_loop(0, 8, finish, 0)
        local.wait()
        other.wait()


def first_pick(picks, bins, gains, weight, inputs):
    anywhere = pl.BlockSpec(memory_space=pl.ANY)
    dma = pltpu.SemaphoreType.DMA
    return pl.pallas_call(
        first_body,
        grid=(8,),
        in_specs=[
            pl.BlockSpec(memory_space=pltpu.SMEM),
            pl.BlockSpec((8, 128), lambda h: (h, 0)),
            pl.BlockSpec((4, 8, 128), lambda h: (0, h, 0)),
            pl.BlockSpec((1024, HALF), lambda h: (h, 0)),
            pl.BlockSpec((MICRO, 32, 1024), lambda h: (0, 0, h)),
        ],
        out_specs=[anywhere, anywhere, anywhere],
        out_shape=[
            jax.ShapeDtypeStruct((2, D, HALF), BF16),
            jax.ShapeDtypeStruct((2, 3, KV, HALF), BF16),
            jax.ShapeDtypeStruct((2, MICRO, ROWS, HALF), F32),
        ],
        scratch_shapes=[
            pltpu.VMEM((8, GROUP, 128), F32),
            pltpu.VMEM((8, GROUP, 128), F32),
            pltpu.VMEM((8, GROUP, 128), F32),
            pltpu.VMEM((8, GROUP, 128), F32),
            pltpu.VMEM((128, 1024), BF16),
            pltpu.VMEM((128, HALF), F32),
            pltpu.VMEM((8, 1024, HALF), BF16),
            pltpu.VMEM((3, KV, HALF), BF16),
            pltpu.VMEM((2, MICRO, ROWS, HALF), F32),
            dma((3, 8)),
            dma((3, 8)),
            dma((3,)),
        ],
        compiler_params=pltpu.CompilerParams(collective_id=3, has_side_effects=True),
        name="first_pick",
    )(picks, bins, gains, weight, inputs)


def deltas_body(picks_ref, bins_ref, w_ref, after_ref, d_ref, wide, back):
    scales_of(bins_ref[...], picks_ref[0, pl.program_id(0)], wide, back)

    def put(rows, columns, value):
        d_ref[0, rows, columns] = value

    for r in range(8):
        quantized(w_ref, wide, back, r, put)


def deltas(count, picks, bins, weight, after):
    return pl.pallas_call(
        deltas_body,
        grid=(count, 8),
        in_specs=[
            pl.BlockSpec(memory_space=pltpu.SMEM),
            pl.BlockSpec((8, 128), lambda p, h: (h, 0)),
            pl.BlockSpec((1024, HALF), lambda p, h: (h, 0)),
            pl.BlockSpec(memory_space=pl.ANY),
        ],
        out_specs=pl.BlockSpec((1, 1024, HALF), lambda p, h: (p, h, 0)),
        out_shape=jax.ShapeDtypeStruct((PICKS, D, HALF), BF16),
        scratch_shapes=[pltpu.VMEM((8, GROUP, 128), F32), pltpu.VMEM((8, GROUP, 128), F32)],
        name="deltas",
    )(picks, bins, weight, after)


def nothing(weight):
    return pl.pallas_call(
        lambda w_ref, d_ref: None,
        in_specs=[pl.BlockSpec(memory_space=pl.ANY)],
        out_specs=pl.BlockSpec(memory_space=pl.ANY),
        out_shape=jax.ShapeDtypeStruct((PICKS, D, HALF), BF16),
        name="nothing",
    )(weight)


def squares(acc):
    total = jnp.sum(jnp.square(acc), axis=0, keepdims=True)
    return total[:, :128] + total[:, 128:256] + total[:, 256:384] + total[:, 384:]


def fused_body(low, picks_ref, bins_ref, w_ref, s_ref, o_ref, wide, back, made, acc):
    pick = low + pl.program_id(0)
    head = pl.program_id(1)
    scales_of(bins_ref[...], picks_ref[0, pick], wide, back)

    @pl.when(head == 0)
    def _():
        acc[...] = jnp.zeros_like(acc)

    def put(rows, columns, value):
        made[rows, columns] = value

    for part in range(2):
        for r in range(4):
            quantized(w_ref, wide, back, part * 4 + r, put)
        rows = slice(part * 512, part * 512 + 512)
        acc[...] += jnp.dot(s_ref[0, :, rows], made[rows, :], preferred_element_type=F32)

    @pl.when(head == 7)
    def _():
        o_ref[pl.ds(pick, 1), :] = squares(acc[...])


def fused(low, picks, bins, weight, stream):
    return pl.pallas_call(
        functools.partial(fused_body, low),
        grid=(PICKS - low, 8),
        in_specs=[
            pl.BlockSpec(memory_space=pltpu.SMEM),
            pl.BlockSpec((8, 128), lambda p, h: (h, 0)),
            pl.BlockSpec((1024, HALF), lambda p, h: (h, 0)),
            pl.BlockSpec((1, 128, 1024), lambda p, h: (lax.div(h, 2), 0, lax.rem(h, 2))),
        ],
        out_specs=pl.BlockSpec((8, 128), lambda p, h: (0, 0)),
        out_shape=jax.ShapeDtypeStruct((8, 128), F32),
        scratch_shapes=[
            pltpu.VMEM((8, GROUP, 128), F32),
            pltpu.VMEM((8, GROUP, 128), F32),
            pltpu.VMEM((1024, HALF), BF16),
            pltpu.VMEM((128, HALF), F32),
        ],
        name="fused",
    )(picks, bins, weight, stream)


def losses_body(s_ref, d_ref, o_ref, acc):
    part = pl.program_id(1)
    product = jnp.dot(s_ref[part], d_ref[0], preferred_element_type=F32)

    @pl.when(part == 0)
    def _():
        acc[...] = product

    @pl.when(part > 0)
    def _():
        acc[...] += product

    @pl.when(part == pl.num_programs(1) - 1)
    def _():
        o_ref[pl.ds(pl.program_id(0), 1), :] = squares(acc[...])


def losses(count, stream, delta):
    depth = 2048
    parts = D // depth
    return pl.pallas_call(
        losses_body,
        grid=(count, parts),
        in_specs=[
            pl.BlockSpec((parts, 128, depth), lambda p, k: (0, 0, 0)),
            pl.BlockSpec((1, depth, HALF), lambda p, k: (p, k, 0)),
        ],
        out_specs=pl.BlockSpec((8, 128), lambda p, k: (0, 0)),
        out_shape=jax.ShapeDtypeStruct((8, 128), F32),
        scratch_shapes=[pltpu.VMEM((128, HALF), F32)],
        name="losses",
    )(stream, delta)


def gains_body(own_ref, o_ref, got, send_sem, recv_sem):
    sections = lax.axis_size("section")
    sec = lax.axis_index("section")
    for i in range(3):
        @pl.when(sec <= i)
        def _():
            got[i] = jnp.ones_like(own_ref)

    barrier = pltpu.get_barrier_semaphore()
    count = jnp.int32(0)
    for step in (1, 2, 3):
        @pl.when(sec + step < sections)
        def _():
            pl.semaphore_signal(barrier, inc=1, device_id={"section": sec + step}, device_id_type=MESH)

        @pl.when(sec >= step)
        def _():
            pl.semaphore_signal(barrier, inc=1, device_id={"section": sec - step}, device_id_type=MESH)

        count = count + jnp.where(sec + step < sections, 1, 0) + jnp.where(sec >= step, 1, 0)
    pl.semaphore_wait(barrier, count)

    def copy(i):
        return pltpu.make_async_remote_copy(
            src_ref=own_ref, dst_ref=got.at[i], send_sem=send_sem.at[i], recv_sem=recv_sem.at[i],
            device_id={"section": jnp.minimum(sec + i + 1, sections - 1)}, device_id_type=MESH,
        )

    for i in range(3):
        @pl.when(sec + i + 1 < sections)
        def _():
            copy(i).start()

    for i in range(3):
        @pl.when(sec > i)
        def _():
            copy(i).wait_recv()

    g1 = got[0]
    g12 = g1 * got[1]
    o_ref[0] = g12 * got[2]
    o_ref[1] = g12
    o_ref[2] = g1
    o_ref[3] = own_ref[...]
    for i in range(3):
        @pl.when(sec + i + 1 < sections)
        def _():
            copy(i).wait_send()


def gains_of(own):
    return pl.pallas_call(
        gains_body,
        in_specs=[pl.BlockSpec(memory_space=pltpu.VMEM)],
        out_specs=pl.BlockSpec(memory_space=pltpu.VMEM),
        out_shape=jax.ShapeDtypeStruct((4, D // 128, 128), F32),
        scratch_shapes=[
            pltpu.VMEM((3, D // 128, 128), F32),
            pltpu.SemaphoreType.DMA((3,)),
            pltpu.SemaphoreType.DMA((3,)),
        ],
        compiler_params=pltpu.CompilerParams(collective_id=2, has_side_effects=True),
        name="gains",
    )(own)


def reduce_body(x_ref, o_ref, slots, send_sem, recv_sem):
    dp, mp = lax.axis_size("dp"), lax.axis_size("mp")
    peers = dp * mp
    rank = lax.axis_index("dp") * mp + lax.axis_index("mp")
    barrier = pltpu.get_barrier_semaphore()

    def place(k):
        other = lax.rem(rank + k, peers)
        return {"dp": lax.div(other, mp), "mp": lax.rem(other, mp)}

    for k in range(1, peers):
        pl.semaphore_signal(barrier, inc=1, device_id=place(k), device_id_type=MESH)
    pl.semaphore_wait(barrier, peers - 1)
    slots[0] = x_ref[...]
    copies = []
    for k in range(1, peers):
        copy = pltpu.make_async_remote_copy(
            src_ref=x_ref,
            dst_ref=slots.at[k],
            send_sem=send_sem.at[k],
            recv_sem=recv_sem.at[k],
            device_id=place(k),
            device_id_type=MESH,
        )
        copy.start()
        copies.append(copy)
    for copy in copies:
        copy.wait()
    total = jnp.zeros_like(o_ref)
    for source in range(peers):
        total = total + slots[lax.rem(rank - source + peers, peers)]
    o_ref[...] = total


def reduce_all(part):
    return pl.pallas_call(
        reduce_body,
        in_specs=[pl.BlockSpec(memory_space=pltpu.VMEM)],
        out_specs=pl.BlockSpec(memory_space=pltpu.VMEM),
        out_shape=jax.ShapeDtypeStruct((8, 128), F32),
        scratch_shapes=[
            pltpu.VMEM((8, 8, 128), F32),
            pltpu.SemaphoreType.DMA((8,)),
            pltpu.SemaphoreType.DMA((8,)),
        ],
        compiler_params=pltpu.CompilerParams(collective_id=1, has_side_effects=True),
        name="reduce_all",
    )(part)


def chain_body(
    x_ref, q_ref, m_ref, a_ref, v_ref, after_ref,
    out_ref, s_ref,
    full, fold, start, bulk, ahead, seen, near, mine,
    q_sem, m_sem, a_sem, x_sem, next_send, next_recv, near_send, near_recv, bulk_send, bulk_recv, save_sem, pair_send, pair_recv,
):
    sections = lax.axis_size("section")
    sec = lax.axis_index("section")
    half = lax.axis_index("mp")
    root = 1.0 / math.sqrt(sections)
    partner = {"mp": 1 - half}

    for i in range(3):
        @pl.when(sec <= i)
        def _():
            near[i] = jnp.zeros_like(near.at[i])

    own_rows = pl.ds(pl.multiple_of(half * ROWS, ROWS), ROWS)
    x_copy = pltpu.make_async_copy(x_ref.at[:, own_rows, :], bulk, x_sem)
    a_copy = pltpu.make_async_copy(a_ref, start, a_sem)
    m_copy = pltpu.make_async_copy(m_ref, fold, m_sem)
    q_copy = pltpu.make_async_copy(q_ref, full, q_sem)
    a_copy.start()

    @pl.when(sec < 4)
    def _():
        x_copy.start()

    m_copy.start()

    @pl.when(sec >= 4)
    def _():
        q_copy.start()

    barrier = pltpu.get_barrier_semaphore()
    pl.semaphore_signal(barrier, inc=1, device_id=partner, device_id_type=MESH)
    count = jnp.int32(1)
    for step in (1, 2, 3, 4):
        @pl.when(sec + step < sections)
        def _():
            pl.semaphore_signal(barrier, inc=1, device_id={"section": sec + step}, device_id_type=MESH)

        @pl.when(sec >= step)
        def _():
            pl.semaphore_signal(barrier, inc=1, device_id={"section": sec - step}, device_id_type=MESH)

        count = count + jnp.where(sec + step < sections, 1, 0) + jnp.where(sec >= step, 1, 0)
    pl.semaphore_wait(barrier, count)

    a_copy.wait()

    @pl.when(sec < 4)
    def _():
        x_copy.wait()

    m_copy.wait()

    @pl.when(sec >= 4)
    def _():
        q_copy.wait()

    def next_copy(part, w, target):
        cols = slice(part * HALF, part * HALF + HALF)
        return pltpu.make_async_remote_copy(
            src_ref=mine.at[w, :, cols], dst_ref=near.at[0, w, :, cols], send_sem=next_send.at[part, w],
            recv_sem=next_recv.at[part, w], device_id=target, device_id_type=MESH,
        )

    def near_copy(i, w, target):
        return pltpu.make_async_remote_copy(
            src_ref=mine.at[w], dst_ref=near.at[i, w], send_sem=near_send.at[i, w],
            recv_sem=near_recv.at[i, w], device_id=target, device_id_type=MESH,
        )

    def bulk_copy(w, target):
        return pltpu.make_async_remote_copy(
            src_ref=ahead.at[w], dst_ref=bulk.at[w], send_sem=bulk_send.at[w],
            recv_sem=bulk_recv.at[w], device_id=target, device_id_type=MESH,
        )

    def tail_copies(w):
        own_cols = pl.ds(pl.multiple_of(half * HALF, HALF), HALF)
        other_cols = pl.ds(pl.multiple_of((1 - half) * HALF, HALF), HALF)
        return (
            pltpu.make_async_copy(mine.at[w, :, own_cols], out_ref.at[w, own_rows, :], save_sem.at[0, w]),
            pltpu.make_async_copy(seen.at[w], s_ref.at[:, w, own_rows, :], save_sem.at[1, w]),
        ), (
            pltpu.make_async_remote_copy(
                src_ref=mine.at[w, :, other_cols], dst_ref=out_ref.at[w, own_rows, :],
                send_sem=pair_send.at[0, w], recv_sem=pair_recv.at[0, w],
                device_id=partner, device_id_type=MESH,
            ),
            pltpu.make_async_remote_copy(
                src_ref=seen.at[w], dst_ref=s_ref.at[:, w, own_rows, :],
                send_sem=pair_send.at[1, w], recv_sem=pair_recv.at[1, w],
                device_id=partner, device_id_type=MESH,
            ),
        )

    def wave(w, carry):
        def deep(k, sums):
            cs = pl.ds(pl.multiple_of(k * 1024, 1024), 1024)
            piece = jnp.concatenate([
                (
                    bulk[w, :, pl.ds(pl.multiple_of(k * 1024 + r * HEAD, HEAD), HEAD)].astype(F32)
                    * v_ref[0, pl.ds(k * 8 + r, 1), :]
                ).astype(BF16)
                for r in range(8)
            ], axis=1)
            return (
                sums[0] + jnp.dot(piece, full[0, cs, :], preferred_element_type=F32),
                sums[1] + jnp.dot(piece, full[1, cs, :], preferred_element_type=F32),
            )

        def from_bulk():
            bulk_copy(w, {"section": sec}).wait_recv()
            zero = jnp.zeros((ROWS, HALF), F32)
            return lax.fori_loop(0, 8, deep, (zero, zero))

        def from_start():
            return (start[0, w], start[1, w])

        sums = lax.cond(sec >= 4, from_bulk, from_start)
        for i in (2, 1):
            def more(sums, i=i):
                near_copy(i, w, {"section": sec}).wait_recv()
                piece = near[i, w]
                return (
                    sums[0] + jnp.dot(piece, fold[0, i], preferred_element_type=F32),
                    sums[1] + jnp.dot(piece, fold[1, i], preferred_element_type=F32),
                )

            sums = lax.cond(sec > i, more, lambda sums: sums, sums)

        def send(part, value):
            mine[w, :, part * HALF : part * HALF + HALF] = value.astype(BF16)

            @pl.when(sec + 1 < sections)
            def _():
                next_copy(part, w, {"section": sec + 1}).start()

        def last(sums):
            next_copy(0, w, {"section": sec}).wait_recv()
            piece = near[0, w, :, :HALF]
            sums = (
                sums[0] + jnp.dot(piece, fold[0, 0, :HALF, :], preferred_element_type=F32),
                sums[1] + jnp.dot(piece, fold[1, 0, :HALF, :], preferred_element_type=F32),
            )
            next_copy(1, w, {"section": sec}).wait_recv()
            piece = near[0, w, :, HALF:]
            send(0, sums[0] + jnp.dot(piece, fold[0, 0, HALF:, :], preferred_element_type=F32))
            send(1, sums[1] + jnp.dot(piece, fold[1, 0, HALF:, :], preferred_element_type=F32))

        @pl.when(sec > 0)
        def _():
            last(sums)

        @pl.when(sec == 0)
        def _():
            send(0, sums[0])
            send(1, sums[1])

        for i in (1, 2):
            @pl.when(sec + i + 1 < sections)
            def _():
                near_copy(i, w, {"section": sec + i + 1}).start()

        def assemble(c, carry):
            heads = pl.ds(pl.multiple_of(c * HEAD, HEAD), HEAD)
            y1 = near[0, w, :, heads].astype(F32) * root
            y2 = near[1, w, :, heads].astype(F32) * root
            y3 = near[2, w, :, heads].astype(F32) * root
            y0 = mine[w, :, heads].astype(F32) * root
            for r in range(8):
                cs = pl.ds(pl.multiple_of(c * 1024 + r * HEAD, HEAD), HEAD)
                row = pl.ds(c * 8 + r, 1)
                now = v_ref[0, row, :] * bulk[w, :, cs].astype(F32) + v_ref[1, row, :] * y3 + v_ref[2, row, :] * y2 + y1
                spot = pl.ds(pl.multiple_of(lax.rem(c, 2) * 1024 + r * HEAD, HEAD), HEAD)
                seen[w, lax.div(c, 2), :, spot] = now.astype(BF16)
                ahead[w, :, cs] = (v_ref[3, row, :] * now + y0).astype(BF16)
            return carry

        lax.fori_loop(0, 8, assemble, 0)

        @pl.when(sec + 4 < sections)
        def _():
            bulk_copy(w, {"section": sec + 4}).start()

        local, remote = tail_copies(w)
        for copy in remote + local:
            copy.start()
        return carry

    lax.fori_loop(0, MICRO, wave, 0)

    def finish(w, carry):
        @pl.when(sec + 1 < sections)
        def _():
            next_copy(0, w, {"section": sec + 1}).wait_send()
            next_copy(1, w, {"section": sec + 1}).wait_send()

        for i in (1, 2):
            @pl.when(sec + i + 1 < sections)
            def _():
                near_copy(i, w, {"section": sec + i + 1}).wait_send()

        @pl.when(sec + 4 < sections)
        def _():
            bulk_copy(w, {"section": sec + 4}).wait_send()

        local, remote = tail_copies(w)
        for copy in local:
            copy.wait()
        for copy in remote:
            copy.wait()
        return carry

    lax.fori_loop(0, MICRO, finish, 0)

def chain(inputs, quant, folds, first, vectors, after):
    anywhere = pl.BlockSpec(memory_space=pl.ANY)
    dma = pltpu.SemaphoreType.DMA
    return pl.pallas_call(
        chain_body,
        in_specs=[anywhere, anywhere, anywhere, anywhere, pl.BlockSpec(memory_space=pltpu.VMEM), anywhere],
        out_specs=[anywhere, anywhere],
        out_shape=[
            jax.ShapeDtypeStruct((MICRO, 32, HALF), BF16),
            jax.ShapeDtypeStruct((4, MICRO, 32, D // 4), BF16),
        ],
        scratch_shapes=[
            pltpu.VMEM((2, D, HALF), BF16),
            pltpu.VMEM((2, 3, KV, HALF), BF16),
            pltpu.VMEM((2, MICRO, ROWS, HALF), F32),
            pltpu.VMEM((MICRO, ROWS, D), BF16),
            pltpu.VMEM((MICRO, ROWS, D), BF16),
            pltpu.VMEM((MICRO, 4, ROWS, D // 4), BF16),
            pltpu.VMEM((3, MICRO, ROWS, KV), BF16),
            pltpu.VMEM((MICRO, ROWS, KV), BF16),
            dma,
            dma,
            dma,
            dma,
            dma((2, MICRO)),
            dma((2, MICRO)),
            dma((3, MICRO)),
            dma((3, MICRO)),
            dma((MICRO,)),
            dma((MICRO,)),
            dma((2, MICRO)),
            dma((2, MICRO)),
            dma((2, MICRO)),
        ],
        compiler_params=pltpu.CompilerParams(
            collective_id=0, has_side_effects=True, vmem_limit_bytes=60 * 1024 * 1024
        ),
        name="chain",
    )(inputs, quant, folds, first, vectors, after)


def local(inputs, value_weight, carry_gain, channel_bins, grid_picks):
    sec = lax.axis_index("section")
    weight = value_weight[0]
    bins = channel_bins.reshape(D // 128, 128)
    gains = gains_of(carry_gain.reshape(D // 128, 128))
    quant, folds, first = first_pick(grid_picks, bins, gains, weight, inputs)
    count = sum(jnp.where(sec >= least, 1, 0) for least in BEFORE).astype(jnp.int32)
    counts = range(PICKS + 1)
    delta = lax.switch(count, [
        functools.partial(deltas, n, grid_picks, bins, weight, first) if n else lambda: nothing(first)
        for n in counts
    ])
    quant_out, stream = chain(inputs, quant, folds, first, gains, delta)
    stream = stream.reshape(4, MICRO * 32, D // 4)
    blank = jnp.zeros((8, 128), F32)
    before, later = lax.switch(count, [
        functools.partial(
            lambda n: (
                losses(n, stream, delta) if n else blank,
                fused(n, grid_picks, bins, weight, stream) if n < PICKS else blank,
            ),
            n,
        )
        for n in counts
    ])
    part = jnp.where(jnp.arange(8)[:, None] < count, before, later)
    total = reduce_all(part)
    entry_count = inputs.shape[0] * inputs.shape[1] * lax.axis_size("dp") * KV
    grid_loss = jnp.sum(total[:PICKS], axis=1) * (LOSS_UNIT / entry_count)
    return (quant_out[None], grid_loss[None])


def solution(mesh):
    placed = (
        P(None, "dp", None),
        P("section", None, "mp"),
        P("section", None),
        P("section", None),
        P("section", None),
    )
    return jax.shard_map(
        local,
        mesh=mesh,
        in_specs=placed,
        out_specs=(P("section", None, "dp", "mp"), P("section", None)),
        check_vma=False,
    )
```

```python
import functools
import math

import jax
import jax.numpy as jnp
from jax import lax
from jax.experimental import pallas as pl
from jax.experimental.pallas import tpu as pltpu
from jax.sharding import PartitionSpec as P

D = 8192
KV = 1024
HALF = 512
HEAD = 128
GROUP = 128
GRID = 20
PICKS = 4
MICRO = 4
ROWS = 16
BEFORE = (9, 14, 20, 25)

EPS = 1e-06
LOSS_UNIT = 1000.0
MESH = pl.DeviceIdType.MESH
SINE = (
    0.9999996039221354,
    -6.579691570017649,
    12.98643600013728,
    -12.188101534445755,
    6.558042246424786,
    -1.953032018015784,
)
F32 = jnp.float32
BF16 = jnp.bfloat16


def sine_part(levels):
    r = levels - jnp.round(levels)
    z = r * r
    acc = jnp.full_like(z, SINE[-1])
    for c in SINE[-2::-1]:
        acc = acc * z + c
    return acc * r


def high_of(w_ref, wide, r, cs):
    high = None
    for q in range(4):
        part = w_ref[r * GROUP + 32 * q : r * GROUP + 32 * q + 32, cs].astype(F32)
        part = jnp.abs(part * wide[r, 32 * q : 32 * q + 32, :])
        part = jnp.max(part, axis=0, keepdims=True)
        high = part if high is None else jnp.maximum(high, part)
    return high + EPS


def quantized(w_ref, wide, back, r, put):
    for c in range(4):
        cs = slice(c * 128, c * 128 + 128)
        high = high_of(w_ref, wide, r, cs)
        up = 7.0 / high
        down = high * (-1.0 / 7.0)
        for q in range(4):
            rows = slice(32 * q, 32 * q + 32)
            at = slice(r * GROUP + 32 * q, r * GROUP + 32 * q + 32)
            w = w_ref[at, cs].astype(F32)
            put(at, cs, rounding_part(w, wide[r, rows, :], back[r, rows, :], up, down).astype(BF16))


def scales_of(bins, pick, wide, back):
    exponent = jnp.full(bins.shape, pick, jnp.int32).astype(F32) / GRID
    scaling = jnp.exp2(exponent * bins.astype(F32) / 4.0)
    columns, inverse = scaling.T, (1.0 / scaling).T
    for r in range(8):
        wide[r] = jnp.broadcast_to(columns[:, r : r + 1], (GROUP, 128))
        back[r] = jnp.broadcast_to(inverse[:, r : r + 1], (GROUP, 128))


def rounding_part(w, scale, back, up, down):
    return sine_part(w * scale * up) * down * back


def first_body(
    picks_ref, bins_ref, g_ref, w_ref, x_ref,
    q_ref, m_ref, a_ref,
    wide, back, near_gain, far_gain, left, acc, made, folds, first,
    q_sem, m_sem, a_sem,
):
    head = pl.program_id(0)
    half = lax.axis_index("mp")
    partner = {"mp": 1 - half}

    def pieces(h):
        at = pl.ds(pl.multiple_of(h * 1024, 1024), 1024)
        src = made.at[h]
        rows = pl.ds(pl.multiple_of(h * HEAD, HEAD), HEAD)
        return (
            pltpu.make_async_copy(src, q_ref.at[half, at, :], q_sem.at[0, h]),
            pltpu.make_async_copy(folds.at[:, rows, :], m_ref.at[half, :, rows, :], m_sem.at[0, h]),
            pltpu.make_async_remote_copy(
                src_ref=folds.at[:, rows, :], dst_ref=m_ref.at[half, :, rows, :],
                send_sem=m_sem.at[1, h], recv_sem=m_sem.at[2, h], device_id=partner, device_id_type=MESH,
            ),
            pltpu.make_async_remote_copy(
                src_ref=src, dst_ref=q_ref.at[half, at, :],
                send_sem=q_sem.at[1, h], recv_sem=q_sem.at[2, h], device_id=partner, device_id_type=MESH,
            ),
        )

    @pl.when(head == 0)
    def _():
        barrier = pltpu.get_barrier_semaphore()
        pl.semaphore_signal(barrier, inc=1, device_id=partner, device_id_type=MESH)
        pl.semaphore_wait(barrier, 1)
        acc[...] = jnp.zeros_like(acc)

    scales_of(bins_ref[...], picks_ref[0, 0], wide, back)
    near_columns, far_columns = g_ref[2].T, g_ref[1].T
    for r in range(8):
        near_gain[r] = jnp.broadcast_to(near_columns[:, r : r + 1], (GROUP, 128))
        far_gain[r] = jnp.broadcast_to(far_columns[:, r : r + 1], (GROUP, 128))
        cs = slice(r * HEAD, r * HEAD + HEAD)
        for w in range(MICRO):
            left[w * 32 : w * 32 + 32, cs] = (x_ref[w, :, cs].astype(F32) * g_ref[0, r : r + 1, :]).astype(BF16)

    head_rows = pl.multiple_of(head * HEAD, HEAD)
    root = 1.0 / math.sqrt(32.0)
    for c in range(4):
        cs = slice(c * 128, c * 128 + 128)
        highs = [high_of(w_ref, wide, r, cs) for r in range(8)]
        ups = [7.0 / high for high in highs]
        downs = [high * (-1.0 / 7.0) for high in highs]
        for q in range(4):
            rows = slice(32 * q, 32 * q + 32)
            sums = None
            for r in range(8):
                at = slice(r * GROUP + 32 * q, r * GROUP + 32 * q + 32)
                w = w_ref[at, cs].astype(F32)
                value = w + rounding_part(w, wide[r, rows, :], back[r, rows, :], ups[r], downs[r])
                made[head, at, cs] = value.astype(BF16)
                terms = (value, value * near_gain[r, rows, :], value * far_gain[r, rows, :])
                sums = terms if sums is None else tuple(x + y for x, y in zip(sums, terms))
            for i in range(3):
                folds[i, pl.ds(head_rows + 32 * q, 32), cs] = (sums[i] * root).astype(BF16)
        if c % 2:
            half_cols = slice(c * 128 - 128, c * 128 + 128)
            acc[:, half_cols] += jnp.dot(left[...], made[head, :, half_cols], preferred_element_type=F32)
    for copy in pieces(head):
        copy.start()

    @pl.when(head == 7)
    def _():
        for side in range(2):
            for w in range(MICRO):
                at = w * 32 + side * ROWS
                first[side, w] = acc[at : at + ROWS, :]
        local = pltpu.make_async_copy(first.at[half], a_ref.at[half], a_sem.at[0])
        other = pltpu.make_async_remote_copy(
            src_ref=first.at[1 - half], dst_ref=a_ref.at[half], send_sem=a_sem.at[1], recv_sem=a_sem.at[2],
            device_id=partner, device_id_type=MESH,
        )
        other.start()
        local.start()

        def finish(h, carry):
            for copy in pieces(h):
                copy.wait()
            return carry

        lax.fori_loop(0, 8, finish, 0)
        local.wait()
        other.wait()


def first_pick(picks, bins, gains, weight, inputs):
    anywhere = pl.BlockSpec(memory_space=pl.ANY)
    dma = pltpu.SemaphoreType.DMA
    return pl.pallas_call(
        first_body,
        grid=(8,),
        in_specs=[
            pl.BlockSpec(memory_space=pltpu.SMEM),
            pl.BlockSpec((8, 128), lambda h: (h, 0)),
            pl.BlockSpec((4, 8, 128), lambda h: (0, h, 0)),
            pl.BlockSpec((1024, HALF), lambda h: (h, 0)),
            pl.BlockSpec((MICRO, 32, 1024), lambda h: (0, 0, h)),
        ],
        out_specs=[anywhere, anywhere, anywhere],
        out_shape=[
            jax.ShapeDtypeStruct((2, D, HALF), BF16),
            jax.ShapeDtypeStruct((2, 3, KV, HALF), BF16),
            jax.ShapeDtypeStruct((2, MICRO, ROWS, HALF), F32),
        ],
        scratch_shapes=[
            pltpu.VMEM((8, GROUP, 128), F32),
            pltpu.VMEM((8, GROUP, 128), F32),
            pltpu.VMEM((8, GROUP, 128), F32),
            pltpu.VMEM((8, GROUP, 128), F32),
            pltpu.VMEM((128, 1024), BF16),
            pltpu.VMEM((128, HALF), F32),
            pltpu.VMEM((8, 1024, HALF), BF16),
            pltpu.VMEM((3, KV, HALF), BF16),
            pltpu.VMEM((2, MICRO, ROWS, HALF), F32),
            dma((3, 8)),
            dma((3, 8)),
            dma((3,)),
        ],
        compiler_params=pltpu.CompilerParams(collective_id=3, has_side_effects=True),
        name="first_pick",
    )(picks, bins, gains, weight, inputs)


def deltas_body(low, picks_ref, bins_ref, w_ref, after_ref, d_ref, wide, back):
    scales_of(bins_ref[...], picks_ref[0, low + pl.program_id(0)], wide, back)

    def put(rows, columns, value):
        d_ref[0, rows, columns] = value

    for r in range(8):
        quantized(w_ref, wide, back, r, put)


def deltas(low, count, picks, bins, weight, after):
    return pl.pallas_call(
        functools.partial(deltas_body, low),
        grid=(count, 8),
        in_specs=[
            pl.BlockSpec(memory_space=pltpu.SMEM),
            pl.BlockSpec((8, 128), lambda p, h: (h, 0)),
            pl.BlockSpec((1024, HALF), lambda p, h: (h, 0)),
            pl.BlockSpec(memory_space=pl.ANY),
        ],
        out_specs=pl.BlockSpec((1, 1024, HALF), lambda p, h: (p, h, 0)),
        out_shape=jax.ShapeDtypeStruct((PICKS, D, HALF), BF16),
        scratch_shapes=[pltpu.VMEM((8, GROUP, 128), F32), pltpu.VMEM((8, GROUP, 128), F32)],
        name="deltas",
    )(picks, bins, weight, after)


def nothing(weight):
    return pl.pallas_call(
        lambda w_ref, d_ref: None,
        in_specs=[pl.BlockSpec(memory_space=pl.ANY)],
        out_specs=pl.BlockSpec(memory_space=pl.ANY),
        out_shape=jax.ShapeDtypeStruct((PICKS, D, HALF), BF16),
        name="nothing",
    )(weight)


def squares(acc):
    total = jnp.sum(jnp.square(acc), axis=0, keepdims=True)
    return total[:, :128] + total[:, 128:256] + total[:, 256:384] + total[:, 384:]


def losses_body(s_ref, *refs):
    *d_refs, o_ref, acc = refs
    half = pl.program_id(1)
    product = sum(
        jnp.dot(
            s_ref[2 * half + k // 2, :, (k % 2) * 1024 : (k % 2) * 1024 + 1024],
            d_refs[k][0],
            preferred_element_type=F32,
        )
        for k in range(4)
    )

    @pl.when(half == 0)
    def _():
        acc[...] = product

    @pl.when(half == 1)
    def _():
        o_ref[pl.ds(pl.program_id(0), 1), :] = squares(acc[...] + product)


def losses(count, stream, delta):
    def piece(k):
        return pl.BlockSpec((1, 1024, HALF), lambda p, h: (p, h * 4 + k, 0))

    return pl.pallas_call(
        losses_body,
        grid=(count, 2),
        in_specs=[pl.BlockSpec((4, 128, 2048), lambda p, h: (0, 0, 0)), *(piece(k) for k in range(4))],
        out_specs=pl.BlockSpec((8, 128), lambda p, h: (0, 0)),
        out_shape=jax.ShapeDtypeStruct((8, 128), F32),
        scratch_shapes=[pltpu.VMEM((128, HALF), F32)],
        name="losses",
    )(stream, delta, delta, delta, delta)


def gains_body(own_ref, o_ref, got, send_sem, recv_sem):
    sections = lax.axis_size("section")
    sec = lax.axis_index("section")
    for i in range(3):
        @pl.when(sec <= i)
        def _():
            got[i] = jnp.ones_like(own_ref)

    barrier = pltpu.get_barrier_semaphore()
    count = jnp.int32(0)
    for step in (1, 2, 3):
        @pl.when(sec + step < sections)
        def _():
            pl.semaphore_signal(barrier, inc=1, device_id={"section": sec + step}, device_id_type=MESH)

        @pl.when(sec >= step)
        def _():
            pl.semaphore_signal(barrier, inc=1, device_id={"section": sec - step}, device_id_type=MESH)

        count = count + jnp.where(sec + step < sections, 1, 0) + jnp.where(sec >= step, 1, 0)
    pl.semaphore_wait(barrier, count)

    def copy(i):
        return pltpu.make_async_remote_copy(
            src_ref=own_ref, dst_ref=got.at[i], send_sem=send_sem.at[i], recv_sem=recv_sem.at[i],
            device_id={"section": jnp.minimum(sec + i + 1, sections - 1)}, device_id_type=MESH,
        )

    for i in range(3):
        @pl.when(sec + i + 1 < sections)
        def _():
            copy(i).start()

    for i in range(3):
        @pl.when(sec > i)
        def _():
            copy(i).wait_recv()

    g1 = got[0]
    g12 = g1 * got[1]
    o_ref[0] = g12 * got[2]
    o_ref[1] = g12
    o_ref[2] = g1
    o_ref[3] = own_ref[...]
    for i in range(3):
        @pl.when(sec + i + 1 < sections)
        def _():
            copy(i).wait_send()


def gains_of(own):
    return pl.pallas_call(
        gains_body,
        in_specs=[pl.BlockSpec(memory_space=pltpu.VMEM)],
        out_specs=pl.BlockSpec(memory_space=pltpu.VMEM),
        out_shape=jax.ShapeDtypeStruct((4, D // 128, 128), F32),
        scratch_shapes=[
            pltpu.VMEM((3, D // 128, 128), F32),
            pltpu.SemaphoreType.DMA((3,)),
            pltpu.SemaphoreType.DMA((3,)),
        ],
        compiler_params=pltpu.CompilerParams(collective_id=2, has_side_effects=True),
        name="gains",
    )(own)


def reduce_body(unit, x_ref, o_ref, slots, send_sem, recv_sem):
    dp, mp = lax.axis_size("dp"), lax.axis_size("mp")
    peers = dp * mp
    rank = lax.axis_index("dp") * mp + lax.axis_index("mp")
    barrier = pltpu.get_barrier_semaphore()

    def place(k):
        other = lax.rem(rank + k, peers)
        return {"dp": lax.div(other, mp), "mp": lax.rem(other, mp)}

    for k in range(1, peers):
        pl.semaphore_signal(barrier, inc=1, device_id=place(k), device_id_type=MESH)
    pl.semaphore_wait(barrier, peers - 1)
    slots[0] = x_ref[...]
    copies = []
    for k in range(1, peers):
        copy = pltpu.make_async_remote_copy(
            src_ref=x_ref,
            dst_ref=slots.at[k],
            send_sem=send_sem.at[k],
            recv_sem=recv_sem.at[k],
            device_id=place(k),
            device_id_type=MESH,
        )
        copy.start()
        copies.append(copy)
    for copy in copies:
        copy.wait()
    total = jnp.zeros_like(x_ref)
    for source in range(peers):
        total = total + slots[lax.rem(rank - source + peers, peers)]
    total = jnp.sum(total, axis=1, keepdims=True) * unit
    o_ref[...] = jnp.broadcast_to(total, (8, 128)).T[0:1, 0:PICKS]


def reduce_all(unit, part):
    return pl.pallas_call(
        functools.partial(reduce_body, unit),
        in_specs=[pl.BlockSpec(memory_space=pltpu.VMEM)],
        out_specs=pl.BlockSpec(memory_space=pltpu.VMEM),
        out_shape=jax.ShapeDtypeStruct((1, PICKS), F32),
        scratch_shapes=[
            pltpu.VMEM((8, 8, 128), F32),
            pltpu.SemaphoreType.DMA((8,)),
            pltpu.SemaphoreType.DMA((8,)),
        ],
        compiler_params=pltpu.CompilerParams(collective_id=1, has_side_effects=True),
        name="reduce_all",
    )(part)


def chain_body(
    x_ref, q_ref, m_ref, a_ref, v_ref, after_ref,
    out_ref, s_ref,
    full, fold, start, bulk, ahead, seen, near, mine,
    q_sem, m_sem, a_sem, x_sem, next_send, next_recv, near_send, near_recv, bulk_send, bulk_recv, save_sem, pair_send, pair_recv,
):
    sections = lax.axis_size("section")
    sec = lax.axis_index("section")
    half = lax.axis_index("mp")
    root = 1.0 / math.sqrt(sections)
    partner = {"mp": 1 - half}

    for i in range(3):
        @pl.when(sec <= i)
        def _():
            near[i] = jnp.zeros_like(near.at[i])

    own_rows = pl.ds(pl.multiple_of(half * ROWS, ROWS), ROWS)
    x_copy = pltpu.make_async_copy(x_ref.at[:, own_rows, :], bulk, x_sem)
    a_copy = pltpu.make_async_copy(a_ref, start, a_sem)
    m_copy = pltpu.make_async_copy(m_ref, fold, m_sem)
    q_copy = pltpu.make_async_copy(q_ref, full, q_sem)
    a_copy.start()

    @pl.when(sec < 4)
    def _():
        x_copy.start()

    m_copy.start()

    @pl.when(sec >= 4)
    def _():
        q_copy.start()

    barrier = pltpu.get_barrier_semaphore()
    pl.semaphore_signal(barrier, inc=1, device_id=partner, device_id_type=MESH)
    count = jnp.int32(1)
    for step in (1, 2, 3, 4):
        @pl.when(sec + step < sections)
        def _():
            pl.semaphore_signal(barrier, inc=1, device_id={"section": sec + step}, device_id_type=MESH)

        @pl.when(sec >= step)
        def _():
            pl.semaphore_signal(barrier, inc=1, device_id={"section": sec - step}, device_id_type=MESH)

        count = count + jnp.where(sec + step < sections, 1, 0) + jnp.where(sec >= step, 1, 0)
    pl.semaphore_wait(barrier, count)

    a_copy.wait()

    @pl.when(sec < 4)
    def _():
        x_copy.wait()

    m_copy.wait()

    @pl.when(sec >= 4)
    def _():
        q_copy.wait()

    def next_copy(part, w, target):
        cols = slice(part * HALF, part * HALF + HALF)
        return pltpu.make_async_remote_copy(
            src_ref=mine.at[w, :, cols], dst_ref=near.at[0, w, :, cols], send_sem=next_send.at[part, w],
            recv_sem=next_recv.at[part, w], device_id=target, device_id_type=MESH,
        )

    def near_copy(i, w, target):
        return pltpu.make_async_remote_copy(
            src_ref=mine.at[w], dst_ref=near.at[i, w], send_sem=near_send.at[i, w],
            recv_sem=near_recv.at[i, w], device_id=target, device_id_type=MESH,
        )

    def bulk_copy(part, w, target):
        cols = pl.ds(pl.multiple_of(part * 2048, 2048), 2048)
        return pltpu.make_async_remote_copy(
            src_ref=ahead.at[w, :, cols], dst_ref=bulk.at[w, :, cols], send_sem=bulk_send.at[part, w],
            recv_sem=bulk_recv.at[part, w], device_id=target, device_id_type=MESH,
        )

    def tail_copies(w):
        own_cols = pl.ds(pl.multiple_of(half * HALF, HALF), HALF)
        other_cols = pl.ds(pl.multiple_of((1 - half) * HALF, HALF), HALF)
        return (
            pltpu.make_async_copy(mine.at[w, :, own_cols], out_ref.at[w, own_rows, :], save_sem.at[0, w]),
            pltpu.make_async_copy(seen.at[w], s_ref.at[:, w, own_rows, :], save_sem.at[1, w]),
        ), (
            pltpu.make_async_remote_copy(
                src_ref=mine.at[w, :, other_cols], dst_ref=out_ref.at[w, own_rows, :],
                send_sem=pair_send.at[0, w], recv_sem=pair_recv.at[0, w],
                device_id=partner, device_id_type=MESH,
            ),
            pltpu.make_async_remote_copy(
                src_ref=seen.at[w], dst_ref=s_ref.at[:, w, own_rows, :],
                send_sem=pair_send.at[1, w], recv_sem=pair_recv.at[1, w],
                device_id=partner, device_id_type=MESH,
            ),
        )

    def wave(w, carry):
        def deep(k, sums):
            cs = pl.ds(pl.multiple_of(k * 1024, 1024), 1024)
            piece = jnp.concatenate([
                (
                    bulk[w, :, pl.ds(pl.multiple_of(k * 1024 + r * HEAD, HEAD), HEAD)].astype(F32)
                    * v_ref[0, pl.ds(k * 8 + r, 1), :]
                ).astype(BF16)
                for r in range(8)
            ], axis=1)
            return (
                sums[0] + jnp.dot(piece, full[0, cs, :], preferred_element_type=F32),
                sums[1] + jnp.dot(piece, full[1, cs, :], preferred_element_type=F32),
            )

        def deep_part(part, sums):
            bulk_copy(part, w, {"section": sec}).wait_recv()
            return lax.fori_loop(2 * part, 2 * part + 2, deep, sums)

        def from_bulk():
            zero = jnp.zeros((ROWS, HALF), F32)
            return lax.fori_loop(0, 4, deep_part, (zero, zero))

        def from_start():
            return (start[0, w], start[1, w])

        sums = lax.cond(sec >= 4, from_bulk, from_start)
        for i in (2, 1):
            def more(sums, i=i):
                near_copy(i, w, {"section": sec}).wait_recv()
                piece = near[i, w]
                return (
                    sums[0] + jnp.dot(piece, fold[0, i], preferred_element_type=F32),
                    sums[1] + jnp.dot(piece, fold[1, i], preferred_element_type=F32),
                )

            sums = lax.cond(sec > i, more, lambda sums: sums, sums)

        def send(part, value):
            mine[w, :, part * HALF : part * HALF + HALF] = value.astype(BF16)

            @pl.when(sec + 1 < sections)
            def _():
                next_copy(part, w, {"section": sec + 1}).start()

        def last(sums):
            next_copy(0, w, {"section": sec}).wait_recv()
            piece = near[0, w, :, :HALF]
            sums = (
                sums[0] + jnp.dot(piece, fold[0, 0, :HALF, :], preferred_element_type=F32),
                sums[1] + jnp.dot(piece, fold[1, 0, :HALF, :], preferred_element_type=F32),
            )
            next_copy(1, w, {"section": sec}).wait_recv()
            piece = near[0, w, :, HALF:]
            send(0, sums[0] + jnp.dot(piece, fold[0, 0, HALF:, :], preferred_element_type=F32))
            send(1, sums[1] + jnp.dot(piece, fold[1, 0, HALF:, :], preferred_element_type=F32))

        @pl.when(sec > 0)
        def _():
            last(sums)

        @pl.when(sec == 0)
        def _():
            send(0, sums[0])
            send(1, sums[1])

        for i in (1, 2):
            @pl.when(sec + i + 1 < sections)
            def _():
                near_copy(i, w, {"section": sec + i + 1}).start()

        def assemble(c, carry):
            heads = pl.ds(pl.multiple_of(c * HEAD, HEAD), HEAD)
            y1 = near[0, w, :, heads].astype(F32) * root
            y2 = near[1, w, :, heads].astype(F32) * root
            y3 = near[2, w, :, heads].astype(F32) * root
            y0 = mine[w, :, heads].astype(F32) * root
            for r in range(8):
                cs = pl.ds(pl.multiple_of(c * 1024 + r * HEAD, HEAD), HEAD)
                row = pl.ds(c * 8 + r, 1)
                now = v_ref[0, row, :] * bulk[w, :, cs].astype(F32) + v_ref[1, row, :] * y3 + v_ref[2, row, :] * y2 + y1
                spot = pl.ds(pl.multiple_of(lax.rem(c, 2) * 1024 + r * HEAD, HEAD), HEAD)
                seen[w, lax.div(c, 2), :, spot] = now.astype(BF16)
                ahead[w, :, cs] = (v_ref[3, row, :] * now + y0).astype(BF16)
            return carry

        def assemble_part(part, carry):
            lax.fori_loop(2 * part, 2 * part + 2, assemble, 0)

            @pl.when(sec + 4 < sections)
            def _():
                bulk_copy(part, w, {"section": sec + 4}).start()

            return carry

        lax.fori_loop(0, 4, assemble_part, 0)

        local, remote = tail_copies(w)
        for copy in remote + local:
            copy.start()
        return carry

    lax.fori_loop(0, MICRO, wave, 0)

    def finish(w, carry):
        @pl.when(sec + 1 < sections)
        def _():
            next_copy(0, w, {"section": sec + 1}).wait_send()
            next_copy(1, w, {"section": sec + 1}).wait_send()

        for i in (1, 2):
            @pl.when(sec + i + 1 < sections)
            def _():
                near_copy(i, w, {"section": sec + i + 1}).wait_send()

        @pl.when(sec + 4 < sections)
        def _():
            for part in range(4):
                bulk_copy(part, w, {"section": sec + 4}).wait_send()

        local, remote = tail_copies(w)
        for copy in local:
            copy.wait()
        for copy in remote:
            copy.wait()
        return carry

    lax.fori_loop(0, MICRO, finish, 0)

def chain(inputs, quant, folds, first, vectors, after):
    anywhere = pl.BlockSpec(memory_space=pl.ANY)
    dma = pltpu.SemaphoreType.DMA
    return pl.pallas_call(
        chain_body,
        in_specs=[anywhere, anywhere, anywhere, anywhere, pl.BlockSpec(memory_space=pltpu.VMEM), anywhere],
        out_specs=[anywhere, anywhere],
        out_shape=[
            jax.ShapeDtypeStruct((MICRO, 32, HALF), BF16),
            jax.ShapeDtypeStruct((4, MICRO, 32, D // 4), BF16),
        ],
        scratch_shapes=[
            pltpu.VMEM((2, D, HALF), BF16),
            pltpu.VMEM((2, 3, KV, HALF), BF16),
            pltpu.VMEM((2, MICRO, ROWS, HALF), F32),
            pltpu.VMEM((MICRO, ROWS, D), BF16),
            pltpu.VMEM((MICRO, ROWS, D), BF16),
            pltpu.VMEM((MICRO, 4, ROWS, D // 4), BF16),
            pltpu.VMEM((3, MICRO, ROWS, KV), BF16),
            pltpu.VMEM((MICRO, ROWS, KV), BF16),
            dma,
            dma,
            dma,
            dma,
            dma((2, MICRO)),
            dma((2, MICRO)),
            dma((3, MICRO)),
            dma((3, MICRO)),
            dma((4, MICRO)),
            dma((4, MICRO)),
            dma((2, MICRO)),
            dma((2, MICRO)),
            dma((2, MICRO)),
        ],
        compiler_params=pltpu.CompilerParams(
            collective_id=0, has_side_effects=True, vmem_limit_bytes=60 * 1024 * 1024
        ),
        name="chain",
    )(inputs, quant, folds, first, vectors, after)


def local(inputs, value_weight, carry_gain, channel_bins, grid_picks):
    sec = lax.axis_index("section")
    weight = value_weight[0]
    bins = channel_bins.reshape(D // 128, 128)
    gains = gains_of(carry_gain.reshape(D // 128, 128))
    quant, folds, first = first_pick(grid_picks, bins, gains, weight, inputs)
    count = sum(jnp.where(sec >= least, 1, 0) for least in BEFORE).astype(jnp.int32)
    counts = range(PICKS + 1)
    delta = lax.switch(count, [
        functools.partial(deltas, 0, n, grid_picks, bins, weight, first) if n else lambda: nothing(first)
        for n in counts
    ])
    quant_out, stream = chain(inputs, quant, folds, first, gains, delta)
    stream = stream.reshape(4, MICRO * 32, D // 4)

    def part(n):
        rest = PICKS - n
        rows = []
        if rest:
            rows.append(losses(rest, stream, deltas(n, rest, grid_picks, bins, weight, stream))[:rest])
        if n:
            rows.insert(0, losses(n, stream, delta)[:n])
        rows.append(jnp.zeros((8 - PICKS, 128), F32))
        return jnp.concatenate(rows)

    total = lax.switch(count, [functools.partial(part, n) for n in counts])
    entry_count = inputs.shape[0] * inputs.shape[1] * lax.axis_size("dp") * KV
    grid_loss = reduce_all(LOSS_UNIT / entry_count, total)
    return (quant_out[None], grid_loss)


def solution(mesh):
    placed = (
        P(None, "dp", None),
        P("section", None, "mp"),
        P("section", None),
        P("section", None),
        P("section", None),
    )
    return jax.shard_map(
        local,
        mesh=mesh,
        in_specs=placed,
        out_specs=(P("section", None, "dp", "mp"), P("section", None)),
        check_vma=False,
    )
```

```python
import functools
import math

import jax
import jax.numpy as jnp
from jax import lax
from jax.experimental import pallas as pl
from jax.experimental.pallas import tpu as pltpu
from jax.sharding import PartitionSpec as P

D = 8192
KV = 1024
HALF = 512
HEAD = 128
GROUP = 128
GRID = 20
PICKS = 4
MICRO = 4
ROWS = 16
BEFORE = (10, 15, 20, 25)

EPS = 1e-06
LOSS_UNIT = 1000.0
MESH = pl.DeviceIdType.MESH
SINE = (
    0.9999996039221354,
    -6.579691570017649,
    12.98643600013728,
    -12.188101534445755,
    6.558042246424786,
    -1.953032018015784,
)
F32 = jnp.float32
BF16 = jnp.bfloat16


def sine_part(levels):
    r = levels - jnp.round(levels)
    z = r * r
    acc = jnp.full_like(z, SINE[-1])
    for c in SINE[-2::-1]:
        acc = acc * z + c
    return acc * r


def high_of(w_ref, wide, r, cs):
    high = None
    for q in range(4):
        part = w_ref[r * GROUP + 32 * q : r * GROUP + 32 * q + 32, cs].astype(F32)
        part = jnp.abs(part * wide[r, 32 * q : 32 * q + 32, :])
        part = jnp.max(part, axis=0, keepdims=True)
        high = part if high is None else jnp.maximum(high, part)
    return high + EPS


def quantized(w_ref, wide, back, r, put):
    for c in range(4):
        cs = slice(c * 128, c * 128 + 128)
        high = high_of(w_ref, wide, r, cs)
        up = 7.0 / high
        down = high * (-1.0 / 7.0)
        for q in range(4):
            rows = slice(32 * q, 32 * q + 32)
            at = slice(r * GROUP + 32 * q, r * GROUP + 32 * q + 32)
            w = w_ref[at, cs].astype(F32)
            put(at, cs, rounding_part(w, wide[r, rows, :], back[r, rows, :], up, down).astype(BF16))


def scales_of(bins, pick, wide, back):
    exponent = jnp.full(bins.shape, pick, jnp.int32).astype(F32) / GRID
    scaling = jnp.exp2(exponent * bins.astype(F32) / 4.0)
    columns, inverse = scaling.T, (1.0 / scaling).T
    for r in range(8):
        wide[r] = jnp.broadcast_to(columns[:, r : r + 1], (GROUP, 128))
        back[r] = jnp.broadcast_to(inverse[:, r : r + 1], (GROUP, 128))


def rounding_part(w, scale, back, up, down):
    return sine_part(w * scale * up) * down * back


def first_body(
    picks_ref, bins_ref, g_ref, w_ref, x_ref,
    q_ref, m_ref, a_ref,
    wide, back, near_gain, far_gain, left, acc, made, folds, first,
    q_sem, m_sem, a_sem,
):
    head = pl.program_id(0)
    half = lax.axis_index("mp")
    partner = {"mp": 1 - half}

    def pieces(h):
        at = pl.ds(pl.multiple_of(h * 1024, 1024), 1024)
        src = made.at[h]
        rows = pl.ds(pl.multiple_of(h * HEAD, HEAD), HEAD)
        return (
            pltpu.make_async_copy(src, q_ref.at[half, at, :], q_sem.at[0, h]),
            pltpu.make_async_copy(folds.at[:, rows, :], m_ref.at[half, :, rows, :], m_sem.at[0, h]),
            pltpu.make_async_remote_copy(
                src_ref=folds.at[:, rows, :], dst_ref=m_ref.at[half, :, rows, :],
                send_sem=m_sem.at[1, h], recv_sem=m_sem.at[2, h], device_id=partner, device_id_type=MESH,
            ),
            pltpu.make_async_remote_copy(
                src_ref=src, dst_ref=q_ref.at[half, at, :],
                send_sem=q_sem.at[1, h], recv_sem=q_sem.at[2, h], device_id=partner, device_id_type=MESH,
            ),
        )

    @pl.when(head == 0)
    def _():
        barrier = pltpu.get_barrier_semaphore()
        pl.semaphore_signal(barrier, inc=1, device_id=partner, device_id_type=MESH)
        pl.semaphore_wait(barrier, 1)
        acc[...] = jnp.zeros_like(acc)

    scales_of(bins_ref[...], picks_ref[0, 0], wide, back)
    near_columns, far_columns = g_ref[2].T, g_ref[1].T
    for r in range(8):
        near_gain[r] = jnp.broadcast_to(near_columns[:, r : r + 1], (GROUP, 128))
        far_gain[r] = jnp.broadcast_to(far_columns[:, r : r + 1], (GROUP, 128))
        cs = slice(r * HEAD, r * HEAD + HEAD)
        for w in range(MICRO):
            left[w * 32 : w * 32 + 32, cs] = (x_ref[w, :, cs].astype(F32) * g_ref[0, r : r + 1, :]).astype(BF16)

    head_rows = pl.multiple_of(head * HEAD, HEAD)
    root = 1.0 / math.sqrt(32.0)
    for c in range(4):
        cs = slice(c * 128, c * 128 + 128)
        highs = [high_of(w_ref, wide, r, cs) for r in range(8)]
        ups = [7.0 / high for high in highs]
        downs = [high * (-1.0 / 7.0) for high in highs]
        for q in range(4):
            rows = slice(32 * q, 32 * q + 32)
            sums = None
            for r in range(8):
                at = slice(r * GROUP + 32 * q, r * GROUP + 32 * q + 32)
                w = w_ref[at, cs].astype(F32)
                value = w + rounding_part(w, wide[r, rows, :], back[r, rows, :], ups[r], downs[r])
                made[head, at, cs] = value.astype(BF16)
                terms = (value, value * near_gain[r, rows, :], value * far_gain[r, rows, :])
                sums = terms if sums is None else tuple(x + y for x, y in zip(sums, terms))
            for i in range(3):
                folds[i, pl.ds(head_rows + 32 * q, 32), cs] = (sums[i] * root).astype(BF16)
        if c % 2:
            half_cols = slice(c * 128 - 128, c * 128 + 128)
            acc[:, half_cols] += jnp.dot(left[...], made[head, :, half_cols], preferred_element_type=F32)
    for copy in pieces(head):
        copy.start()

    @pl.when(head == 7)
    def _():
        for side in range(2):
            for w in range(MICRO):
                at = w * 32 + side * ROWS
                first[side, w] = acc[at : at + ROWS, :]
        local = pltpu.make_async_copy(first.at[half], a_ref.at[half], a_sem.at[0])
        other = pltpu.make_async_remote_copy(
            src_ref=first.at[1 - half], dst_ref=a_ref.at[half], send_sem=a_sem.at[1], recv_sem=a_sem.at[2],
            device_id=partner, device_id_type=MESH,
        )
        other.start()
        local.start()

        def finish(h, carry):
            for copy in pieces(h):
                copy.wait()
            return carry

        lax.fori_loop(0, 8, finish, 0)
        local.wait()
        other.wait()


def first_pick(picks, bins, gains, weight, inputs):
    anywhere = pl.BlockSpec(memory_space=pl.ANY)
    dma = pltpu.SemaphoreType.DMA
    return pl.pallas_call(
        first_body,
        grid=(8,),
        in_specs=[
            pl.BlockSpec(memory_space=pltpu.SMEM),
            pl.BlockSpec((8, 128), lambda h: (h, 0)),
            pl.BlockSpec((4, 8, 128), lambda h: (0, h, 0)),
            pl.BlockSpec((1024, HALF), lambda h: (h, 0)),
            pl.BlockSpec((MICRO, 32, 1024), lambda h: (0, 0, h)),
        ],
        out_specs=[anywhere, anywhere, anywhere],
        out_shape=[
            jax.ShapeDtypeStruct((2, D, HALF), BF16),
            jax.ShapeDtypeStruct((2, 3, KV, HALF), BF16),
            jax.ShapeDtypeStruct((2, MICRO, ROWS, HALF), F32),
        ],
        scratch_shapes=[
            pltpu.VMEM((8, GROUP, 128), F32),
            pltpu.VMEM((8, GROUP, 128), F32),
            pltpu.VMEM((8, GROUP, 128), F32),
            pltpu.VMEM((8, GROUP, 128), F32),
            pltpu.VMEM((128, 1024), BF16),
            pltpu.VMEM((128, HALF), F32),
            pltpu.VMEM((8, 1024, HALF), BF16),
            pltpu.VMEM((3, KV, HALF), BF16),
            pltpu.VMEM((2, MICRO, ROWS, HALF), F32),
            dma((3, 8)),
            dma((3, 8)),
            dma((3,)),
        ],
        compiler_params=pltpu.CompilerParams(collective_id=3, has_side_effects=True),
        name="first_pick",
    )(picks, bins, gains, weight, inputs)


def deltas_body(low, picks_ref, bins_ref, w_ref, after_ref, d_ref, wide, back):
    scales_of(bins_ref[...], picks_ref[0, low + pl.program_id(0)], wide, back)

    def put(rows, columns, value):
        d_ref[0, rows, columns] = value

    for r in range(8):
        quantized(w_ref, wide, back, r, put)


def deltas(low, count, picks, bins, weight, after):
    return pl.pallas_call(
        functools.partial(deltas_body, low),
        grid=(count, 8),
        in_specs=[
            pl.BlockSpec(memory_space=pltpu.SMEM),
            pl.BlockSpec((8, 128), lambda p, h: (h, 0)),
            pl.BlockSpec((1024, HALF), lambda p, h: (h, 0)),
            pl.BlockSpec(memory_space=pl.ANY),
        ],
        out_specs=pl.BlockSpec((1, 1024, HALF), lambda p, h: (p, h, 0)),
        out_shape=jax.ShapeDtypeStruct((PICKS, D, HALF), BF16),
        scratch_shapes=[pltpu.VMEM((8, GROUP, 128), F32), pltpu.VMEM((8, GROUP, 128), F32)],
        name="deltas",
    )(picks, bins, weight, after)


def nothing(weight):
    return pl.pallas_call(
        lambda w_ref, d_ref: None,
        in_specs=[pl.BlockSpec(memory_space=pl.ANY)],
        out_specs=pl.BlockSpec(memory_space=pl.ANY),
        out_shape=jax.ShapeDtypeStruct((PICKS, D, HALF), BF16),
        name="nothing",
    )(weight)


def squares(acc):
    total = jnp.sum(jnp.square(acc), axis=0, keepdims=True)
    return total[:, :128] + total[:, 128:256] + total[:, 256:384] + total[:, 384:]


def losses_body(s_ref, *refs):
    *d_refs, o_ref, acc = refs
    half = pl.program_id(1)
    product = sum(
        jnp.dot(
            s_ref[2 * half + k // 2, :, (k % 2) * 1024 : (k % 2) * 1024 + 1024],
            d_refs[k][0],
            preferred_element_type=F32,
        )
        for k in range(4)
    )

    @pl.when(half == 0)
    def _():
        acc[...] = product

    @pl.when(half == 1)
    def _():
        o_ref[pl.ds(pl.program_id(0), 1), :] = squares(acc[...] + product)


def losses(count, stream, delta):
    def piece(k):
        return pl.BlockSpec((1, 1024, HALF), lambda p, h: (p, h * 4 + k, 0))

    return pl.pallas_call(
        losses_body,
        grid=(count, 2),
        in_specs=[pl.BlockSpec((4, 128, 2048), lambda p, h: (0, 0, 0)), *(piece(k) for k in range(4))],
        out_specs=pl.BlockSpec((8, 128), lambda p, h: (0, 0)),
        out_shape=jax.ShapeDtypeStruct((8, 128), F32),
        scratch_shapes=[pltpu.VMEM((128, HALF), F32)],
        name="losses",
    )(stream, delta, delta, delta, delta)


def gains_body(own_ref, o_ref, got, send_sem, recv_sem):
    sections = lax.axis_size("section")
    sec = lax.axis_index("section")
    for i in range(3):
        @pl.when(sec <= i)
        def _():
            got[i] = jnp.ones_like(own_ref)

    barrier = pltpu.get_barrier_semaphore()
    count = jnp.int32(0)
    for step in (1, 2, 3):
        @pl.when(sec + step < sections)
        def _():
            pl.semaphore_signal(barrier, inc=1, device_id={"section": sec + step}, device_id_type=MESH)

        @pl.when(sec >= step)
        def _():
            pl.semaphore_signal(barrier, inc=1, device_id={"section": sec - step}, device_id_type=MESH)

        count = count + jnp.where(sec + step < sections, 1, 0) + jnp.where(sec >= step, 1, 0)
    pl.semaphore_wait(barrier, count)

    def copy(i):
        return pltpu.make_async_remote_copy(
            src_ref=own_ref, dst_ref=got.at[i], send_sem=send_sem.at[i], recv_sem=recv_sem.at[i],
            device_id={"section": jnp.minimum(sec + i + 1, sections - 1)}, device_id_type=MESH,
        )

    for i in range(3):
        @pl.when(sec + i + 1 < sections)
        def _():
            copy(i).start()

    for i in range(3):
        @pl.when(sec > i)
        def _():
            copy(i).wait_recv()

    g1 = got[0]
    g12 = g1 * got[1]
    o_ref[0] = g12 * got[2]
    o_ref[1] = g12
    o_ref[2] = g1
    o_ref[3] = own_ref[...]
    for i in range(3):
        @pl.when(sec + i + 1 < sections)
        def _():
            copy(i).wait_send()


def gains_of(own):
    return pl.pallas_call(
        gains_body,
        in_specs=[pl.BlockSpec(memory_space=pltpu.VMEM)],
        out_specs=pl.BlockSpec(memory_space=pltpu.VMEM),
        out_shape=jax.ShapeDtypeStruct((4, D // 128, 128), F32),
        scratch_shapes=[
            pltpu.VMEM((3, D // 128, 128), F32),
            pltpu.SemaphoreType.DMA((3,)),
            pltpu.SemaphoreType.DMA((3,)),
        ],
        compiler_params=pltpu.CompilerParams(collective_id=2, has_side_effects=True),
        name="gains",
    )(own)


def reduce_body(unit, x_ref, o_ref, slots, send_sem, recv_sem):
    dp, mp = lax.axis_size("dp"), lax.axis_size("mp")
    peers = dp * mp
    rank = lax.axis_index("dp") * mp + lax.axis_index("mp")
    barrier = pltpu.get_barrier_semaphore()

    def place(k):
        other = lax.rem(rank + k, peers)
        return {"dp": lax.div(other, mp), "mp": lax.rem(other, mp)}

    for k in range(1, peers):
        pl.semaphore_signal(barrier, inc=1, device_id=place(k), device_id_type=MESH)
    pl.semaphore_wait(barrier, peers - 1)
    slots[0] = x_ref[...]
    copies = []
    for k in range(1, peers):
        copy = pltpu.make_async_remote_copy(
            src_ref=x_ref,
            dst_ref=slots.at[k],
            send_sem=send_sem.at[k],
            recv_sem=recv_sem.at[k],
            device_id=place(k),
            device_id_type=MESH,
        )
        copy.start()
        copies.append(copy)
    for copy in copies:
        copy.wait()
    total = jnp.zeros_like(x_ref)
    for source in range(peers):
        total = total + slots[lax.rem(rank - source + peers, peers)]
    total = jnp.sum(total, axis=1, keepdims=True) * unit
    o_ref[...] = jnp.broadcast_to(total, (8, 128)).T[0:1, 0:PICKS]


def reduce_all(unit, part):
    return pl.pallas_call(
        functools.partial(reduce_body, unit),
        in_specs=[pl.BlockSpec(memory_space=pltpu.VMEM)],
        out_specs=pl.BlockSpec(memory_space=pltpu.VMEM),
        out_shape=jax.ShapeDtypeStruct((1, PICKS), F32),
        scratch_shapes=[
            pltpu.VMEM((8, 8, 128), F32),
            pltpu.SemaphoreType.DMA((8,)),
            pltpu.SemaphoreType.DMA((8,)),
        ],
        compiler_params=pltpu.CompilerParams(collective_id=1, has_side_effects=True),
        name="reduce_all",
    )(part)


def chain_body(
    x_ref, q_ref, m_ref, a_ref, v_ref, after_ref,
    out_ref, s_ref,
    full, fold, start, bulk, ahead, seen, near, mine,
    q_sem, m_sem, a_sem, x_sem, next_send, next_recv, near_send, near_recv, bulk_send, bulk_recv, save_sem, pair_send, pair_recv,
):
    sections = lax.axis_size("section")
    sec = lax.axis_index("section")
    half = lax.axis_index("mp")
    root = 1.0 / math.sqrt(sections)
    partner = {"mp": 1 - half}

    for i in range(3):
        @pl.when(sec <= i)
        def _():
            near[i] = jnp.zeros_like(near.at[i])

    own_rows = pl.ds(pl.multiple_of(half * ROWS, ROWS), ROWS)
    x_copy = pltpu.make_async_copy(x_ref.at[:, own_rows, :], bulk, x_sem)
    a_copy = pltpu.make_async_copy(a_ref, start, a_sem)
    m_copy = pltpu.make_async_copy(m_ref, fold, m_sem)
    q_copy = pltpu.make_async_copy(q_ref, full, q_sem)
    a_copy.start()

    @pl.when(sec < 4)
    def _():
        x_copy.start()

    m_copy.start()

    @pl.when(sec >= 4)
    def _():
        q_copy.start()

    barrier = pltpu.get_barrier_semaphore()
    pl.semaphore_signal(barrier, inc=1, device_id=partner, device_id_type=MESH)
    count = jnp.int32(1)
    for step in (1, 2, 3, 4):
        @pl.when(sec + step < sections)
        def _():
            pl.semaphore_signal(barrier, inc=1, device_id={"section": sec + step}, device_id_type=MESH)

        @pl.when(sec >= step)
        def _():
            pl.semaphore_signal(barrier, inc=1, device_id={"section": sec - step}, device_id_type=MESH)

        count = count + jnp.where(sec + step < sections, 1, 0) + jnp.where(sec >= step, 1, 0)
    pl.semaphore_wait(barrier, count)

    a_copy.wait()

    @pl.when(sec >= 1)
    def _():
        m_copy.wait()

    @pl.when(sec >= 4)
    def _():
        q_copy.wait()

    def next_copy(part, w, target):
        cols = slice(part * HALF, part * HALF + HALF)
        return pltpu.make_async_remote_copy(
            src_ref=mine.at[w, :, cols], dst_ref=near.at[0, w, :, cols], send_sem=next_send.at[part, w],
            recv_sem=next_recv.at[part, w], device_id=target, device_id_type=MESH,
        )

    def near_copy(i, w, target):
        return pltpu.make_async_remote_copy(
            src_ref=mine.at[w], dst_ref=near.at[i, w], send_sem=near_send.at[i, w],
            recv_sem=near_recv.at[i, w], device_id=target, device_id_type=MESH,
        )

    def bulk_copy(part, w, target):
        cols = pl.ds(pl.multiple_of(part * 2048, 2048), 2048)
        return pltpu.make_async_remote_copy(
            src_ref=ahead.at[w, :, cols], dst_ref=bulk.at[w, :, cols], send_sem=bulk_send.at[part, w],
            recv_sem=bulk_recv.at[part, w], device_id=target, device_id_type=MESH,
        )

    def tail_copies(w):
        own_cols = pl.ds(pl.multiple_of(half * HALF, HALF), HALF)
        other_cols = pl.ds(pl.multiple_of((1 - half) * HALF, HALF), HALF)
        return (
            pltpu.make_async_copy(mine.at[w, :, own_cols], out_ref.at[w, own_rows, :], save_sem.at[0, w]),
            pltpu.make_async_copy(seen.at[w], s_ref.at[:, w, own_rows, :], save_sem.at[1, w]),
        ), (
            pltpu.make_async_remote_copy(
                src_ref=mine.at[w, :, other_cols], dst_ref=out_ref.at[w, own_rows, :],
                send_sem=pair_send.at[0, w], recv_sem=pair_recv.at[0, w],
                device_id=partner, device_id_type=MESH,
            ),
            pltpu.make_async_remote_copy(
                src_ref=seen.at[w], dst_ref=s_ref.at[:, w, own_rows, :],
                send_sem=pair_send.at[1, w], recv_sem=pair_recv.at[1, w],
                device_id=partner, device_id_type=MESH,
            ),
        )

    def wave(w, carry):
        def deep(k, sums):
            cs = pl.ds(pl.multiple_of(k * 1024, 1024), 1024)
            piece = jnp.concatenate([
                (
                    bulk[w, :, pl.ds(pl.multiple_of(k * 1024 + r * HEAD, HEAD), HEAD)].astype(F32)
                    * v_ref[0, pl.ds(k * 8 + r, 1), :]
                ).astype(BF16)
                for r in range(8)
            ], axis=1)
            return (
                sums[0] + jnp.dot(piece, full[0, cs, :], preferred_element_type=F32),
                sums[1] + jnp.dot(piece, full[1, cs, :], preferred_element_type=F32),
            )

        def deep_part(part, sums):
            bulk_copy(part, w, {"section": sec}).wait_recv()
            return lax.fori_loop(2 * part, 2 * part + 2, deep, sums)

        def from_bulk():
            zero = jnp.zeros((ROWS, HALF), F32)
            return lax.fori_loop(0, 4, deep_part, (zero, zero))

        def from_start():
            return (start[0, w], start[1, w])

        sums = lax.cond(sec >= 4, from_bulk, from_start)
        for i in (2, 1):
            def more(sums, i=i):
                near_copy(i, w, {"section": sec}).wait_recv()
                piece = near[i, w]
                return (
                    sums[0] + jnp.dot(piece, fold[0, i], preferred_element_type=F32),
                    sums[1] + jnp.dot(piece, fold[1, i], preferred_element_type=F32),
                )

            sums = lax.cond(sec > i, more, lambda sums: sums, sums)

        def send(part, value):
            mine[w, :, part * HALF : part * HALF + HALF] = value.astype(BF16)

            @pl.when(sec + 1 < sections)
            def _():
                next_copy(part, w, {"section": sec + 1}).start()

        def last(sums):
            next_copy(0, w, {"section": sec}).wait_recv()
            piece = near[0, w, :, :HALF]
            sums = (
                sums[0] + jnp.dot(piece, fold[0, 0, :HALF, :], preferred_element_type=F32),
                sums[1] + jnp.dot(piece, fold[1, 0, :HALF, :], preferred_element_type=F32),
            )
            next_copy(1, w, {"section": sec}).wait_recv()
            piece = near[0, w, :, HALF:]
            send(0, sums[0] + jnp.dot(piece, fold[0, 0, HALF:, :], preferred_element_type=F32))
            send(1, sums[1] + jnp.dot(piece, fold[1, 0, HALF:, :], preferred_element_type=F32))

        @pl.when(sec > 0)
        def _():
            last(sums)

        @pl.when(sec == 0)
        def _():
            send(0, sums[0])
            send(1, sums[1])

        for i in (1, 2):
            @pl.when(sec + i + 1 < sections)
            def _():
                near_copy(i, w, {"section": sec + i + 1}).start()

        @pl.when((sec < 4) & (w == 0))
        def _():
            x_copy.wait()

        def assemble(c, carry):
            heads = pl.ds(pl.multiple_of(c * HEAD, HEAD), HEAD)
            y1 = near[0, w, :, heads].astype(F32) * root
            y2 = near[1, w, :, heads].astype(F32) * root
            y3 = near[2, w, :, heads].astype(F32) * root
            y0 = mine[w, :, heads].astype(F32) * root
            for r in range(8):
                cs = pl.ds(pl.multiple_of(c * 1024 + r * HEAD, HEAD), HEAD)
                row = pl.ds(c * 8 + r, 1)
                now = v_ref[0, row, :] * bulk[w, :, cs].astype(F32) + v_ref[1, row, :] * y3 + v_ref[2, row, :] * y2 + y1
                spot = pl.ds(pl.multiple_of(lax.rem(c, 2) * 1024 + r * HEAD, HEAD), HEAD)
                seen[w, lax.div(c, 2), :, spot] = now.astype(BF16)
                ahead[w, :, cs] = (v_ref[3, row, :] * now + y0).astype(BF16)
            return carry

        def assemble_part(part, carry):
            lax.fori_loop(2 * part, 2 * part + 2, assemble, 0)

            @pl.when(sec + 4 < sections)
            def _():
                bulk_copy(part, w, {"section": sec + 4}).start()

            return carry

        lax.fori_loop(0, 4, assemble_part, 0)

        local, remote = tail_copies(w)
        for copy in remote + local:
            copy.start()
        return carry

    lax.fori_loop(0, MICRO, wave, 0)

    def finish(w, carry):
        @pl.when(sec + 1 < sections)
        def _():
            next_copy(0, w, {"section": sec + 1}).wait_send()
            next_copy(1, w, {"section": sec + 1}).wait_send()

        for i in (1, 2):
            @pl.when(sec + i + 1 < sections)
            def _():
                near_copy(i, w, {"section": sec + i + 1}).wait_send()

        @pl.when(sec + 4 < sections)
        def _():
            for part in range(4):
                bulk_copy(part, w, {"section": sec + 4}).wait_send()

        local, remote = tail_copies(w)
        for copy in local:
            copy.wait()
        for copy in remote:
            copy.wait()
        return carry

    lax.fori_loop(0, MICRO, finish, 0)

    @pl.when(sec < 1)
    def _():
        m_copy.wait()

def chain(inputs, quant, folds, first, vectors, after):
    anywhere = pl.BlockSpec(memory_space=pl.ANY)
    dma = pltpu.SemaphoreType.DMA
    return pl.pallas_call(
        chain_body,
        in_specs=[anywhere, anywhere, anywhere, anywhere, pl.BlockSpec(memory_space=pltpu.VMEM), anywhere],
        out_specs=[anywhere, anywhere],
        out_shape=[
            jax.ShapeDtypeStruct((MICRO, 32, HALF), BF16),
            jax.ShapeDtypeStruct((4, MICRO, 32, D // 4), BF16),
        ],
        scratch_shapes=[
            pltpu.VMEM((2, D, HALF), BF16),
            pltpu.VMEM((2, 3, KV, HALF), BF16),
            pltpu.VMEM((2, MICRO, ROWS, HALF), F32),
            pltpu.VMEM((MICRO, ROWS, D), BF16),
            pltpu.VMEM((MICRO, ROWS, D), BF16),
            pltpu.VMEM((MICRO, 4, ROWS, D // 4), BF16),
            pltpu.VMEM((3, MICRO, ROWS, KV), BF16),
            pltpu.VMEM((MICRO, ROWS, KV), BF16),
            dma,
            dma,
            dma,
            dma,
            dma((2, MICRO)),
            dma((2, MICRO)),
            dma((3, MICRO)),
            dma((3, MICRO)),
            dma((4, MICRO)),
            dma((4, MICRO)),
            dma((2, MICRO)),
            dma((2, MICRO)),
            dma((2, MICRO)),
        ],
        compiler_params=pltpu.CompilerParams(
            collective_id=0, has_side_effects=True, vmem_limit_bytes=60 * 1024 * 1024
        ),
        name="chain",
    )(inputs, quant, folds, first, vectors, after)


def local(inputs, value_weight, carry_gain, channel_bins, grid_picks):
    sec = lax.axis_index("section")
    weight = value_weight[0]
    bins = channel_bins.reshape(D // 128, 128)
    gains = gains_of(carry_gain.reshape(D // 128, 128))
    quant, folds, first = first_pick(grid_picks, bins, gains, weight, inputs)
    count = sum(jnp.where(sec >= least, 1, 0) for least in BEFORE).astype(jnp.int32)
    counts = range(PICKS + 1)
    delta = lax.switch(count, [
        functools.partial(deltas, 0, n, grid_picks, bins, weight, first) if n else lambda: nothing(first)
        for n in counts
    ])
    quant_out, stream = chain(inputs, quant, folds, first, gains, delta)
    stream = stream.reshape(4, MICRO * 32, D // 4)

    def part(n):
        rest = PICKS - n
        rows = []
        if rest:
            rows.append(losses(rest, stream, deltas(n, rest, grid_picks, bins, weight, stream))[:rest])
        if n:
            rows.insert(0, losses(n, stream, delta)[:n])
        rows.append(jnp.zeros((8 - PICKS, 128), F32))
        return jnp.concatenate(rows)

    total = lax.switch(count, [functools.partial(part, n) for n in counts])
    entry_count = inputs.shape[0] * inputs.shape[1] * lax.axis_size("dp") * KV
    grid_loss = reduce_all(LOSS_UNIT / entry_count, total)
    return (quant_out[None], grid_loss)


def solution(mesh):
    placed = (
        P(None, "dp", None),
        P("section", None, "mp"),
        P("section", None),
        P("section", None),
        P("section", None),
    )
    return jax.shard_map(
        local,
        mesh=mesh,
        in_specs=placed,
        out_specs=(P("section", None, "dp", "mp"), P("section", None)),
        check_vma=False,
    )
```
